8 devices in a mesh: replica: 1 (over z), tp: 2 (over y), stage: 4 (over x, core).
Axes of the slice: x: 2, y: 2, z: 1, core: 2. Of those that a mesh axis runs over, the one named last changes fastest.
Arguments:
- embeds: bfloat16 [48, 16, 2048], P('replica')
- w_qkv: bfloat16 [4, 2048, 16, 3, 128], P('stage', None, 'tp')
- w_out: bfloat16 [4, 2048, 2048], P('stage', 'tp')
- w_gate: bfloat16 [4, 2048, 5504], P('stage', None, 'tp')
- w_up: bfloat16 [4, 2048, 5504], P('stage', None, 'tp')
- w_down: bfloat16 [4, 5504, 2048], P('stage', 'tp')
- norm_gain: float32 [4, 2, 2048], P('stage')
- k_cache: bfloat16 [4, 48, 16, 16, 16, 128], P('stage', 'replica', None, None, 'tp')
- v_cache: bfloat16 [4, 48, 16, 16, 16, 128], P('stage', 'replica', None, None, 'tp')
- lengths: int32 [48, 16], P('replica')
- final_gain: float32 [2048], replicated
- w_unembed: bfloat16 [2048, 32000], P(None, ('stage', 'tp'))
Outputs:
- output 1: float32 [48, 16, 32000], P('replica', None, ('stage', 'tp'))
- output 2: bfloat16 [4, 48, 16, 16, 16, 128], P('stage', 'replica', None, None, 'tp')
- output 3: bfloat16 [4, 48, 16, 16, 16, 128], P('stage', 'replica', None, None, 'tp')
All inputs are finite; a program needn't handle non-finite values.
Results may differ from the reference program's by a relative error of at most 0.02.
Values are sent between devices in bfloat16 or wider.
A program may use at most 1 GiB of HBM per device.

```python
import jax
import jax.numpy as jnp
from jax import lax

D = 2048
HEADS = 16
KV_HEADS = 16
HEAD = 128
FF = 5504
VOCAB = 32000
STAGES = 4
LAYERS_STAGE = 1
GROUPS = 48
BATCH = 16
CTX = 16

LAYERS = LAYERS_STAGE * STAGES
QGROUP = HEADS // KV_HEADS
SLOTS = QGROUP + 2
ROPE_THETA = 10000.0
NORM_EPS = 1e-5


def draw_lengths(len_key):
    low_len = CTX // 4
    tok_count = GROUPS * BATCH
    len_flat = jax.random.randint(len_key, (tok_count,), low_len, CTX, dtype=jnp.int32)
    pick_idx = jax.random.permutation(jax.random.fold_in(len_key, 1), tok_count)
    len_flat = len_flat.at[pick_idx[0]].set(CTX - 1).at[pick_idx[1]].set(low_len)
    return len_flat.reshape(GROUPS, BATCH)


def setup_inputs(seed: int = 0, part: int = 0) -> dict:
    root_key = jax.random.key(seed)
    shared_keys = jax.random.split(root_key, 8)
    part_keys = jax.random.split(jax.random.fold_in(root_key, part), 4)
    embeds = jax.random.normal(part_keys[0], (GROUPS, BATCH, D), jnp.float32).astype(jnp.bfloat16)
    w_qkv = (jax.random.normal(shared_keys[0], (LAYERS, D, KV_HEADS, SLOTS, HEAD), jnp.float32) * D ** -0.5).astype(jnp.bfloat16)
    w_out = (jax.random.normal(shared_keys[1], (LAYERS, HEADS * HEAD, D), jnp.float32) * (HEADS * HEAD) ** -0.5).astype(jnp.bfloat16)
    w_gate = (jax.random.normal(shared_keys[2], (LAYERS, D, FF), jnp.float32) * D ** -0.5).astype(jnp.bfloat16)
    w_up = (jax.random.normal(shared_keys[3], (LAYERS, D, FF), jnp.float32) * D ** -0.5).astype(jnp.bfloat16)
    w_down = (jax.random.normal(shared_keys[4], (LAYERS, FF, D), jnp.float32) * FF ** -0.5).astype(jnp.bfloat16)
    norm_gain = 1.0 + 0.25 * jax.random.normal(shared_keys[5], (LAYERS, 2, D), jnp.float32)
    k_cache = jax.random.normal(part_keys[1], (LAYERS, GROUPS, BATCH, CTX, KV_HEADS, HEAD), jnp.float32).astype(jnp.bfloat16)
    v_cache = jax.random.normal(part_keys[2], (LAYERS, GROUPS, BATCH, CTX, KV_HEADS, HEAD), jnp.float32).astype(jnp.bfloat16)
    lengths = draw_lengths(part_keys[3])
    final_gain = 1.0 + 0.25 * jax.random.normal(shared_keys[6], (D,), jnp.float32)
    w_unembed = (jax.random.normal(shared_keys[7], (D, VOCAB), jnp.float32) * D ** -0.5).astype(jnp.bfloat16)
    return dict(embeds=embeds, w_qkv=w_qkv, w_out=w_out, w_gate=w_gate, w_up=w_up, w_down=w_down, norm_gain=norm_gain, k_cache=k_cache, v_cache=v_cache, lengths=lengths, final_gain=final_gain, w_unembed=w_unembed)


def rms_norm(values, gain_row):
    mean_sq = jnp.mean(values * values, axis=-1, keepdims=True)
    return (values * lax.rsqrt(mean_sq + NORM_EPS) * gain_row).astype(jnp.bfloat16)


def rotate_half(values, cos_part, sin_part):
    half_dim = values.shape[-1] // 2
    first_half = values[..., :half_dim]
    second_half = values[..., half_dim:]
    return jnp.concatenate([first_half * cos_part - second_half * sin_part, second_half * cos_part + first_half * sin_part], axis=-1)


def reference(embeds, w_qkv, w_out, w_gate, w_up, w_down, norm_gain, k_cache, v_cache, lengths, final_gain, w_unembed):
    tok_count = GROUPS * BATCH
    inv_freq = ROPE_THETA ** (-jnp.arange(HEAD // 2, dtype=jnp.float32) * (2.0 / HEAD))
    angles = lengths.astype(jnp.float32)[..., None] * inv_freq
    cos_part = jnp.cos(angles)
    sin_part = jnp.sin(angles)
    cos_q = cos_part[:, :, None, None, :]
    sin_q = sin_part[:, :, None, None, :]
    cos_k = cos_part[:, :, None, :]
    sin_k = sin_part[:, :, None, :]
    positions = jnp.arange(CTX)
    write_hit = (positions[None, None, :] == lengths[:, :, None])[:, :, :, None, None]
    visible = (positions[None, None, :] <= lengths[:, :, None])[:, :, None, None, :]
    stage_end = (jnp.arange(LAYERS) % LAYERS_STAGE) == LAYERS_STAGE - 1

    def layer_step(residual, layer_in):
        wq_layer, wo_layer, wg_layer, wu_layer, wd_layer, gain_pair, k_layer, v_layer, at_end = layer_in
        normed = rms_norm(residual, gain_pair[0]).reshape(tok_count, D)
        proj_out = jnp.dot(normed, wq_layer.reshape(D, KV_HEADS * SLOTS * HEAD), preferred_element_type=jnp.float32)
        proj_out = proj_out.reshape(GROUPS, BATCH, KV_HEADS, SLOTS, HEAD)
        queries = rotate_half(proj_out[:, :, :, :QGROUP], cos_q, sin_q).astype(jnp.bfloat16)
        key_new = rotate_half(proj_out[:, :, :, QGROUP], cos_k, sin_k).astype(jnp.bfloat16)
        val_new = proj_out[:, :, :, QGROUP + 1].astype(jnp.bfloat16)
        k_upd = jnp.where(write_hit, key_new[:, :, None], k_layer)
        v_upd = jnp.where(write_hit, val_new[:, :, None], v_layer)
        scores = jnp.einsum('gbkqn,gbtkn->gbkqt', queries.astype(jnp.float32), k_upd.astype(jnp.float32)) * HEAD ** -0.5
        scores = jnp.where(visible, scores, -jnp.inf)
        attn_probs = jax.nn.softmax(scores, axis=-1).astype(jnp.bfloat16)
        attn_out = jnp.einsum('gbkqt,gbtkn->gbkqn', attn_probs.astype(jnp.float32), v_upd.astype(jnp.float32)).astype(jnp.bfloat16)
        residual = residual + jnp.dot(attn_out.reshape(tok_count, HEADS * HEAD), wo_layer, preferred_element_type=jnp.float32).reshape(GROUPS, BATCH, D)
        normed_mlp = rms_norm(residual, gain_pair[1]).reshape(tok_count, D)
        gate_act = jnp.dot(normed_mlp, wg_layer, preferred_element_type=jnp.float32)
        up_act = jnp.dot(normed_mlp, wu_layer, preferred_element_type=jnp.float32)
        hidden = (jax.nn.silu(gate_act) * up_act).astype(jnp.bfloat16)
        residual = residual + jnp.dot(hidden, wd_layer, preferred_element_type=jnp.float32).reshape(GROUPS, BATCH, D)
        residual = jnp.where(at_end, residual.astype(jnp.bfloat16).astype(jnp.float32), residual)
        return residual, (k_upd, v_upd)

    final_res, cache_pair = lax.scan(layer_step, embeds.astype(jnp.float32), (w_qkv, w_out, w_gate, w_up, w_down, norm_gain, k_cache, v_cache, stage_end))
    normed_out = rms_norm(final_res, final_gain).reshape(tok_count, D)
    logits = jnp.dot(normed_out, w_unembed, preferred_element_type=jnp.float32).reshape(GROUPS, BATCH, VOCAB)
    return logits, cache_pair[0], cache_pair[1]
```

```python
import jax
import jax.numpy as jnp
from jax import lax
from jax.sharding import PartitionSpec as P

NORM_EPS = 1e-5
ROPE_THETA = 10000.0


def rms_norm(values, gain_row):
    mean_sq = jnp.mean(values * values, axis=-1, keepdims=True)
    return (values * lax.rsqrt(mean_sq + NORM_EPS) * gain_row).astype(jnp.bfloat16)


def rotate_half(values, cos_part, sin_part):
    half_dim = values.shape[-1] // 2
    first_half = values[..., :half_dim]
    second_half = values[..., half_dim:]
    return jnp.concatenate([first_half * cos_part - second_half * sin_part, second_half * cos_part + first_half * sin_part], axis=-1)


def rope_tables(lengths, head_dim):
    inv_freq = ROPE_THETA ** (-jnp.arange(head_dim // 2, dtype=jnp.float32) * (2.0 / head_dim))
    angles = lengths.astype(jnp.float32)[..., None] * inv_freq
    return jnp.cos(angles), jnp.sin(angles)


def tp_sum(partial):
    return partial + lax.ppermute(partial.astype(jnp.bfloat16), 'tp', [(0, 1), (1, 0)]).astype(jnp.float32)


def store_group(store_buf, new_rows, group_slot, is_valid, axis_pos):
    kept_rows = lax.dynamic_index_in_dim(store_buf, group_slot, axis_pos, keepdims=False)
    return lax.dynamic_update_index_in_dim(store_buf, jnp.where(is_valid, new_rows, kept_rows), group_slot, axis_pos)


def stage_layers(residual, lengths_row, w_qkv, w_out, w_gate, w_up, w_down, norm_gain, k_group, v_group):
    batch_rows, width = residual.shape
    layer_count = w_qkv.shape[0]
    kv_local = w_qkv.shape[2]
    slot_count = w_qkv.shape[3]
    head_dim = w_qkv.shape[4]
    q_per_kv = slot_count - 2
    cos_part, sin_part = rope_tables(lengths_row, head_dim)
    cos_q = cos_part[:, None, None, :]
    sin_q = sin_part[:, None, None, :]
    cos_k = cos_part[:, None, :]
    sin_k = sin_part[:, None, :]
    visible = (jnp.arange(k_group.shape[2])[None, :] < lengths_row[:, None])[:, None, None, :]
    score_scale = head_dim ** -0.5
    key_rows = []
    val_rows = []
    for layer_idx in range(layer_count):
        normed = rms_norm(residual, norm_gain[layer_idx, 0])
        proj_out = jnp.dot(normed, w_qkv[layer_idx].reshape(width, kv_local * slot_count * head_dim), preferred_element_type=jnp.float32).reshape(batch_rows, kv_local, slot_count, head_dim)
        queries = rotate_half(proj_out[:, :, :q_per_kv], cos_q, sin_q).astype(jnp.bfloat16)
        key_new = rotate_half(proj_out[:, :, q_per_kv], cos_k, sin_k).astype(jnp.bfloat16)
        val_new = proj_out[:, :, q_per_kv + 1].astype(jnp.bfloat16)
        old_scores = jnp.einsum('bkqn,btkn->bkqt', queries, k_group[layer_idx], preferred_element_type=jnp.float32) * score_scale
        old_scores = jnp.where(visible, old_scores, -jnp.inf)
        new_score = jnp.einsum('bkqn,bkn->bkq', queries, key_new, preferred_element_type=jnp.float32) * score_scale
        peak_score = jnp.maximum(jnp.max(old_scores, axis=-1), new_score)
        old_exp = jnp.exp(old_scores - peak_score[..., None])
        new_exp = jnp.exp(new_score - peak_score)
        denom_sum = jnp.sum(old_exp, axis=-1) + new_exp
        old_probs = (old_exp / denom_sum[..., None]).astype(jnp.bfloat16)
        new_probs = (new_exp / denom_sum).astype(jnp.bfloat16)
        attn_out = jnp.einsum('bkqt,btkn->bkqn', old_probs, v_group[layer_idx], preferred_element_type=jnp.float32)
        attn_out = attn_out + jnp.einsum('bkq,bkn->bkqn', new_probs, val_new, preferred_element_type=jnp.float32)
        attn_flat = attn_out.astype(jnp.bfloat16).reshape(batch_rows, kv_local * q_per_kv * head_dim)
        residual = residual + tp_sum(jnp.dot(attn_flat, w_out[layer_idx], preferred_element_type=jnp.float32))
        normed_mlp = rms_norm(residual, norm_gain[layer_idx, 1])
        gate_act = jnp.dot(normed_mlp, w_gate[layer_idx], preferred_element_type=jnp.float32)
        up_act = jnp.dot(normed_mlp, w_up[layer_idx], preferred_element_type=jnp.float32)
        hidden = (jax.nn.silu(gate_act) * up_act).astype(jnp.bfloat16)
        residual = residual + tp_sum(jnp.dot(hidden, w_down[layer_idx], preferred_element_type=jnp.float32))
        key_rows.append(key_new)
        val_rows.append(val_new)
    return residual, jnp.stack(key_rows), jnp.stack(val_rows)


def solution(mesh):
    stages = mesh.shape['stage']
    cache_spec = P('stage', 'replica', None, None, 'tp', None)
    in_specs = (P('replica'), P('stage', None, 'tp', None, None), P('stage', 'tp', None), P('stage', None, 'tp'), P('stage', None, 'tp'), P('stage', 'tp', None), P('stage'), cache_spec, cache_spec, P('replica'), P(), P(None, ('stage', 'tp')))
    out_specs = (P('replica', None, ('stage', 'tp')), cache_spec, cache_spec)
    next_stage = [(src_idx, src_idx + 1) for src_idx in range(stages - 1)]

    def device_step(embeds, w_qkv, w_out, w_gate, w_up, w_down, norm_gain, k_cache, v_cache, lengths, final_gain, w_unembed):
        groups, seqs, width = embeds.shape
        merge = 6
        group_count, batch_rows = groups // merge, seqs * merge
        cache_shape = k_cache.shape
        embeds = embeds.reshape(group_count, batch_rows, width)
        lengths = lengths.reshape(group_count, batch_rows)
        k_cache = k_cache.reshape((cache_shape[0], group_count, batch_rows) + cache_shape[3:])
        v_cache = v_cache.reshape((cache_shape[0], group_count, batch_rows) + cache_shape[3:])
        stage_idx = lax.axis_index('stage')
        row_shape = (k_cache.shape[0], group_count, batch_rows, k_cache.shape[4], k_cache.shape[5])

        def tick_body(tick_idx, loop_state):
            incoming, key_store, val_store, final_rows = loop_state
            group_idx = tick_idx - stage_idx
            is_valid = jnp.logical_and(group_idx >= 0, group_idx < group_count)
            group_slot = jnp.clip(group_idx, 0, group_count - 1)
            first_in = lax.dynamic_index_in_dim(embeds, group_slot, 0, keepdims=False)
            residual = jnp.where(stage_idx == 0, first_in, incoming).astype(jnp.float32)
            lengths_row = lax.dynamic_index_in_dim(lengths, group_slot, 0, keepdims=False)
            k_group = lax.dynamic_index_in_dim(k_cache, group_slot, 1, keepdims=False)
            v_group = lax.dynamic_index_in_dim(v_cache, group_slot, 1, keepdims=False)
            residual, key_rows, val_rows = stage_layers(residual, lengths_row, w_qkv, w_out, w_gate, w_up, w_down, norm_gain, k_group, v_group)
            hidden_out = residual.astype(jnp.bfloat16)
            key_store = store_group(key_store, key_rows, group_slot, is_valid, 1)
            val_store = store_group(val_store, val_rows, group_slot, is_valid, 1)
            final_rows = store_group(final_rows, hidden_out, group_slot, is_valid, 0)
            incoming = lax.ppermute(hidden_out, 'stage', next_stage)
            return incoming, key_store, val_store, final_rows

        start_state = (jnp.zeros((batch_rows, width), jnp.bfloat16), jnp.zeros(row_shape, jnp.bfloat16), jnp.zeros(row_shape, jnp.bfloat16), jnp.zeros((group_count, batch_rows, width), jnp.bfloat16))
        loop_out = lax.fori_loop(0, group_count + stages - 1, tick_body, start_state)
        final_all = lax.psum(jnp.where(stage_idx == stages - 1, loop_out[3], jnp.zeros_like(loop_out[3])), 'stage')
        normed_out = rms_norm(final_all.astype(jnp.float32), final_gain).reshape(group_count * batch_rows, width)
        logits = jnp.dot(normed_out, w_unembed, preferred_element_type=jnp.float32).reshape(groups, seqs, w_unembed.shape[1])
        write_mask = (jnp.arange(k_cache.shape[3])[None, None, :] == lengths[:, :, None])[None, :, :, :, None, None]
        k_out = jnp.where(write_mask, loop_out[1][:, :, :, None], k_cache)
        v_out = jnp.where(write_mask, loop_out[2][:, :, :, None], v_cache)
        return logits, k_out.reshape(cache_shape), v_out.reshape(cache_shape)

    return jax.shard_map(device_step, mesh=mesh, in_specs=in_specs, out_specs=out_specs, check_vma=False)
```

```python
import functools

import jax
import jax.numpy as jnp
from jax import lax
from jax.experimental import pallas as pl
from jax.experimental.pallas import tpu as pltpu
from jax.sharding import PartitionSpec as P

NORM_EPS = 1e-5
ROPE_THETA = 10000.0
MESH = pl.DeviceIdType.MESH
F32 = jnp.float32
BF16 = jnp.bfloat16
MERGE = 3
TAIL_ROWS = 48
VMEM_LIMIT = 67043328


def rms_norm(values, gain_row):
    mean_sq = jnp.mean(values * values, axis=-1, keepdims=True)
    return (values * lax.rsqrt(mean_sq + NORM_EPS) * gain_row).astype(BF16)


def rope_tables(lengths, head_dim):
    inv_freq = ROPE_THETA ** (-jnp.arange(head_dim // 2, dtype=F32) * (2.0 / head_dim))
    angles = lengths.astype(F32)[..., None] * inv_freq
    cos_part, sin_part = jnp.cos(angles), jnp.sin(angles)
    return jnp.concatenate([cos_part, cos_part], -1), jnp.concatenate([-sin_part, sin_part], -1)


def column_chunks(total, width):
    return [(low, min(width, total - low)) for low in range(0, total, width)]


def dot(lhs, rhs):
    return jnp.dot(lhs, rhs, preferred_element_type=F32)


def pipeline_kernel(
    stages, batch, lens_ref, gain_ref, cos_ref, sin_ref, emb_ref, wqkv_hbm, wout_hbm, wgate_hbm, wup_hbm, wdown_hbm, kc_hbm, vc_hbm,
    final_ref, knew_ref, vnew_ref,
    wqkv, wout, wgate, wup, wdown, kbuf, vbuf, xbuf, xout, resid, send_a, recv_a, send_d, recv_d, unit, hidden, attn, q_scr, k_scr, v_scr, o_scr,
    w_sem, c_sem, n_sem, e_sem, a_send, a_recv, d_send, d_recv, x_send, x_recv, f_send, f_recv, credit,
):
    stage = lax.axis_index("stage")
    peer = {"tp": 1 - lax.axis_index("tp")}
    last = stages - 1
    rows = emb_ref.shape[0]
    count = rows // batch
    heads, head_dim = kbuf.shape[2], kbuf.shape[3]
    slots = kbuf.shape[1]
    scale = head_dim ** -0.5
    weights = [pltpu.make_async_copy(src, dst, w_sem.at[i]) for i, (src, dst) in enumerate(
        [(wqkv_hbm, wqkv), (wout_hbm, wout), (wgate_hbm, wgate), (wup_hbm, wup), (wdown_hbm, wdown)])]

    def span(step):
        return pl.ds(pl.multiple_of(step * batch, batch), batch)

    def emb_copy(step):
        return pltpu.make_async_copy(emb_ref.at[span(step)], xbuf.at[lax.rem(step, 2)], e_sem.at[lax.rem(step, 2)])

    def cache_copies(step):
        return (pltpu.make_async_copy(kc_hbm.at[span(step)], kbuf, c_sem.at[0]), pltpu.make_async_copy(vc_hbm.at[span(step)], vbuf, c_sem.at[1]))

    def new_copies(step):
        return (pltpu.make_async_copy(k_scr, knew_ref.at[span(step)], n_sem.at[0]), pltpu.make_async_copy(v_scr, vnew_ref.at[span(step)], n_sem.at[1]))

    def sum_copy(step, send, recv, send_sem, recv_sem):
        slot = lax.rem(step, 2)
        return pltpu.make_async_remote_copy(send.at[slot], recv.at[slot], send_sem.at[slot], recv_sem.at[slot], device_id=peer, device_id_type=MESH)

    def hop_copy(step):
        slot = lax.rem(step, 2)
        return pltpu.make_async_remote_copy(xout.at[slot], xbuf.at[slot], x_send.at[slot], x_recv.at[slot], device_id={"stage": stage + 1}, device_id_type=MESH)

    def final_copies(step):
        slot = lax.rem(step, 2)
        return [pltpu.make_async_remote_copy(xout.at[slot], final_ref.at[span(step)], f_send.at[slot, dst], f_recv.at[step], device_id={"stage": dst}, device_id_type=MESH)
                for dst in range(last)]

    def final_local(step):
        slot = lax.rem(step, 2)
        return pltpu.make_async_copy(xout.at[slot], final_ref.at[span(step)], f_send.at[slot, last])

    for copy in weights[:1] + list(cache_copies(0)) + weights[1:]:
        copy.start()

    @pl.when(stage == 0)
    def _():
        emb_copy(0).start()
        emb_copy(1).start()

    def attend(step):
        slot = lax.rem(step, 2)

        @pl.when(stage == 0)
        def _():
            emb_copy(step).wait()

        @pl.when(stage > 0)
        def _():
            pltpu.make_async_remote_copy(xout.at[slot], xbuf.at[slot], x_send.at[slot], x_recv.at[slot], device_id={"stage": stage}, device_id_type=MESH).wait_recv()

        @pl.when(step == 0)
        def _():
            weights[0].wait()

        @pl.when(step > 0)
        def _():
            for copy in new_copies(step - 1):
                copy.wait()

        unit[...] = rms_norm(xbuf[slot].astype(F32), gain_ref[0:1, :])
        cos_part = cos_ref[span(step), :]
        sin_part = sin_ref[span(step), :]
        for low, width in column_chunks(wqkv.shape[1], 6 * head_dim):
            proj = dot(unit[...], wqkv[:, low:low + width])
            for part in range(width // (3 * head_dim)):
                head = low // (3 * head_dim) + part
                base = part * 3 * head_dim
                query = proj[:, base:base + head_dim]
                key = proj[:, base + head_dim:base + 2 * head_dim]
                q_scr[:, head, :] = (query * cos_part + pltpu.roll(query, head_dim // 2, 1) * sin_part).astype(BF16).astype(F32)
                k_scr[:, head, :] = (key * cos_part + pltpu.roll(key, head_dim // 2, 1) * sin_part).astype(BF16).astype(F32)
                v_scr[:, head, :] = proj[:, base + 2 * head_dim:base + 3 * head_dim].astype(BF16).astype(F32)
        for copy in cache_copies(step):
            copy.wait()
        for copy in new_copies(step):
            copy.start()
        position = lax.broadcasted_iota(jnp.int32, (slots, heads, 1), 0)

        def one_row(row):
            length = lens_ref[step * batch + row]
            query = q_scr[row]
            scores = jnp.sum(query[None] * kbuf[row].astype(F32), axis=-1, keepdims=True) * scale
            scores = jnp.where(position < length, scores, -jnp.inf)
            fresh = jnp.sum(query * k_scr[row], axis=-1, keepdims=True) * scale
            peak = jnp.maximum(jnp.max(scores, axis=0), fresh)
            exps = jnp.exp(scores - peak[None])
            fresh_exp = jnp.exp(fresh - peak)
            inverse = 1.0 / (jnp.sum(exps, axis=0) + fresh_exp)
            probs = (exps * inverse[None]).astype(BF16).astype(F32)
            fresh_prob = (fresh_exp * inverse).astype(BF16).astype(F32)
            o_scr[row] = jnp.sum(probs * vbuf[row].astype(F32), axis=0) + fresh_prob * v_scr[row]

        def rows_body(index, carry):
            for sub in range(2):
                one_row(index * 2 + sub)
            return carry

        lax.fori_loop(0, batch // 2, rows_body, 0)

        @pl.when(step + 1 < count)
        def _():
            for copy in cache_copies(step + 1):
                copy.start()

    def project(step):
        slot = lax.rem(step, 2)

        @pl.when(step == 0)
        def _():
            weights[1].wait()

        for head in range(heads):
            attn[:, head * head_dim:(head + 1) * head_dim] = o_scr[:, head, :].astype(BF16)
        for low, width in column_chunks(wout.shape[1], 1024):
            partial = dot(attn[...], wout[:, low:low + width])
            send_a[slot, :, low:low + width] = partial.astype(BF16)
            resid[slot, :, low:low + width] = xbuf[slot, :, low:low + width].astype(F32) + partial
        sum_copy(step, send_a, recv_a, a_send, a_recv).start()

        @pl.when(jnp.logical_and(stage == 0, step + 2 < count))
        def _():
            emb_copy(step + 2).start()

        @pl.when(jnp.logical_and(stage > 0, step + 2 < count))
        def _():
            pl.semaphore_signal(credit, inc=1, device_id={"stage": stage - 1}, device_id_type=MESH)

    def feed_forward(step):
        slot = lax.rem(step, 2)

        @pl.when(step == 0)
        def _():
            for copy in weights[2:]:
                copy.wait()

        sum_copy(step, send_a, recv_a, a_send, a_recv).wait()
        summed = resid[slot] + recv_a[slot].astype(F32)
        resid[slot] = summed
        unit[...] = rms_norm(summed, gain_ref[1:2, :])
        for low, width in column_chunks(wgate.shape[1], 768):
            gate = dot(unit[...], wgate[:, low:low + width])
            up = dot(unit[...], wup[:, low:low + width])
            hidden[:, low:low + width] = (jax.nn.silu(gate) * up).astype(BF16)
        for low, width in column_chunks(wdown.shape[1], 1024):
            partial = dot(hidden[...], wdown[:, low:low + width])
            send_d[slot, :, low:low + width] = partial.astype(BF16)
            resid[slot, :, low:low + width] = resid[slot, :, low:low + width] + partial
        sum_copy(step, send_d, recv_d, d_send, d_recv).start()

    def hand_on(step):
        slot = lax.rem(step, 2)
        sum_copy(step, send_d, recv_d, d_send, d_recv).wait()

        @pl.when(jnp.logical_and(stage < last, step >= 2))
        def _():
            hop_copy(step - 2).wait_send()
            pl.semaphore_wait(credit, 1)

        @pl.when(jnp.logical_and(stage == last, step >= 2))
        def _():
            for copy in final_copies(step - 2):
                copy.wait_send()
            final_local(step - 2).wait()

        xout[slot] = (resid[slot] + recv_d[slot].astype(F32)).astype(BF16)

        @pl.when(stage < last)
        def _():
            hop_copy(step).start()

        @pl.when(stage == last)
        def _():
            for copy in final_copies(step):
                copy.start()
            final_local(step).start()

    def slot_body(step, carry):
        @pl.when(step < count)
        def _():
            attend(step)

        @pl.when(step >= 2)
        def _():
            hand_on(step - 2)

        @pl.when(step < count)
        def _():
            project(step)

        @pl.when(jnp.logical_and(step >= 1, step <= count))
        def _():
            feed_forward(step - 1)

        return carry

    lax.fori_loop(0, count + 2, slot_body, 0)
    for copy in new_copies(count - 1):
        copy.wait()

    @pl.when(stage < last)
    def _():
        for step in (count - 2, count - 1):
            hop_copy(step).wait_send()

        def drain(step, carry):
            pltpu.make_async_remote_copy(xout.at[0], final_ref.at[span(step)], f_send.at[0, 0], f_recv.at[step], device_id={"stage": stage}, device_id_type=MESH).wait_recv()
            return carry

        lax.fori_loop(0, count, drain, 0)

    @pl.when(stage == last)
    def _():
        for step in (count - 2, count - 1):
            for copy in final_copies(step):
                copy.wait_send()
            final_local(step).wait()


def run_pipeline(stages, lens, gains, cos_part, sin_part, embeds, wqkv, wout, wgate, wup, wdown, k_cache, v_cache):
    rows, width = embeds.shape
    batch = 16 * MERGE
    slots, heads, head_dim = k_cache.shape[1:]
    count = rows // batch
    anywhere = pl.BlockSpec(memory_space=pl.ANY)
    local = pl.BlockSpec(memory_space=pltpu.VMEM)
    pair = pltpu.SemaphoreType.DMA((2,))
    new_rows = jax.ShapeDtypeStruct((rows, heads, head_dim), F32)
    return pl.pallas_call(
        functools.partial(pipeline_kernel, stages, batch),
        out_shape=(jax.ShapeDtypeStruct((rows, width), BF16), new_rows, new_rows),
        in_specs=[pl.BlockSpec(memory_space=pltpu.SMEM), local, local, local] + [anywhere] * 8,
        out_specs=(anywhere, anywhere, anywhere),
        scratch_shapes=[
            pltpu.VMEM(wqkv.shape, BF16), pltpu.VMEM(wout.shape, BF16), pltpu.VMEM(wgate.shape, BF16), pltpu.VMEM(wup.shape, BF16), pltpu.VMEM(wdown.shape, BF16),
            pltpu.VMEM((batch, slots, heads, head_dim), BF16), pltpu.VMEM((batch, slots, heads, head_dim), BF16),
            pltpu.VMEM((2, batch, width), BF16), pltpu.VMEM((2, batch, width), BF16), pltpu.VMEM((2, batch, width), F32),
            pltpu.VMEM((2, batch, width), BF16), pltpu.VMEM((2, batch, width), BF16), pltpu.VMEM((2, batch, width), BF16), pltpu.VMEM((2, batch, width), BF16),
            pltpu.VMEM((batch, width), BF16), pltpu.VMEM((batch, wgate.shape[1]), BF16), pltpu.VMEM((batch, heads * head_dim), BF16),
            pltpu.VMEM((batch, heads, head_dim), F32), pltpu.VMEM((batch, heads, head_dim), F32), pltpu.VMEM((batch, heads, head_dim), F32), pltpu.VMEM((batch, heads, head_dim), F32),
            pltpu.SemaphoreType.DMA((5,)), pair, pair, pair, pair, pair, pair, pair, pair, pair,
            pltpu.SemaphoreType.DMA((2, stages)), pltpu.SemaphoreType.DMA((count,)), pltpu.SemaphoreType.REGULAR,
        ],
        compiler_params=pltpu.CompilerParams(has_side_effects=True, vmem_limit_bytes=VMEM_LIMIT),
    )(lens, gains, cos_part, sin_part, embeds, wqkv, wout, wgate, wup, wdown, k_cache, v_cache)


def tail_kernel(lens_ref, gain_ref, final_ref, knew_ref, vnew_ref, kc_ref, vc_ref, wun_ref, logits_ref, ko_ref, vo_ref):
    block = pl.program_id(0)
    rows = kc_ref.shape[0]
    ko_ref[...] = kc_ref[...]
    vo_ref[...] = vc_ref[...]

    def place(row, carry):
        length = lens_ref[block * rows + row]
        ko_ref[row, length] = knew_ref[row].astype(BF16)
        vo_ref[row, length] = vnew_ref[row].astype(BF16)
        return carry

    lax.fori_loop(0, rows, place, 0)
    normed = rms_norm(final_ref[...].astype(F32), gain_ref[...])
    for low, width in column_chunks(wun_ref.shape[1], 1024):
        logits_ref[:, low:low + width] = dot(normed, wun_ref[:, low:low + width])


def run_tail(lens, gain, final, knew, vnew, k_cache, v_cache, wun):
    rows, width = final.shape
    slots, heads, head_dim = k_cache.shape[1:]
    vocab = wun.shape[1]
    cache_spec = pl.BlockSpec((TAIL_ROWS, slots, heads, head_dim), lambda i, lens: (i, 0, 0, 0))
    new_spec = pl.BlockSpec((TAIL_ROWS, heads, head_dim), lambda i, lens: (i, 0, 0))
    return pl.pallas_call(
        tail_kernel,
        out_shape=(jax.ShapeDtypeStruct((rows, vocab), F32), jax.ShapeDtypeStruct(k_cache.shape, BF16), jax.ShapeDtypeStruct(v_cache.shape, BF16)),
        grid_spec=pltpu.PrefetchScalarGridSpec(
            num_scalar_prefetch=1,
            grid=(rows // TAIL_ROWS,),
            in_specs=[pl.BlockSpec((1, width), lambda i, lens: (0, 0)), pl.BlockSpec((TAIL_ROWS, width), lambda i, lens: (i, 0)), new_spec, new_spec, cache_spec, cache_spec,
                      pl.BlockSpec((width, vocab), lambda i, lens: (0, 0), pipeline_mode=pl.Buffered(1))],
            out_specs=(pl.BlockSpec((TAIL_ROWS, vocab), lambda i, lens: (i, 0)), cache_spec, cache_spec),
        ),
        compiler_params=pltpu.CompilerParams(dimension_semantics=("arbitrary",), vmem_limit_bytes=VMEM_LIMIT),
    )(lens, gain, final, knew, vnew, k_cache, v_cache, wun)


def solution(mesh):
    stages = mesh.shape['stage']
    cache_spec = P('stage', 'replica', None, None, 'tp', None)
    in_specs = (P('replica'), P('stage', None, 'tp', None, None), P('stage', 'tp', None), P('stage', None, 'tp'), P('stage', None, 'tp'), P('stage', 'tp', None), P('stage'), cache_spec, cache_spec, P('replica'), P(), P(None, ('stage', 'tp')))
    out_specs = (P('replica', None, ('stage', 'tp')), cache_spec, cache_spec)

    def device_step(embeds, w_qkv, w_out, w_gate, w_up, w_down, norm_gain, k_cache, v_cache, lengths, final_gain, w_unembed):
        groups, seqs, width = embeds.shape
        rows = groups * seqs
        cache_shape = k_cache.shape
        head_dim = cache_shape[-1]
        lens = lengths.reshape(rows)
        cos_part, sin_part = rope_tables(lens, head_dim)
        k_rows = k_cache.reshape((rows,) + cache_shape[3:])
        v_rows = v_cache.reshape((rows,) + cache_shape[3:])
        final, knew, vnew = run_pipeline(
            stages, lens, norm_gain[0], cos_part, sin_part, embeds.reshape(rows, width), w_qkv[0].reshape(width, -1), w_out[0], w_gate[0], w_up[0], w_down[0], k_rows, v_rows)
        logits, k_out, v_out = run_tail(lens, final_gain.reshape(1, width), final, knew, vnew, k_rows, v_rows, w_unembed)
        return logits.reshape(groups, seqs, -1), k_out.reshape(cache_shape), v_out.reshape(cache_shape)

    return jax.shard_map(device_step, mesh=mesh, in_specs=in_specs, out_specs=out_specs, check_vma=False)
```

```python
import functools

import jax
import jax.numpy as jnp
from jax import lax
from jax.experimental import pallas as pl
from jax.experimental.pallas import tpu as pltpu
from jax.sharding import PartitionSpec as P

NORM_EPS = 1e-5
ROPE_THETA = 10000.0
MESH = pl.DeviceIdType.MESH
F32 = jnp.float32
BF16 = jnp.bfloat16
MERGE = 4
TAIL_STEPS = 16
LOG2_E = 1.4426950408889634
MIN_LENGTH = 4
ROW_UNROLL = 4
VMEM_LIMIT = 67043328


def rms_norm(values, gain_row):
    mean_sq = jnp.mean(values * values, axis=-1, keepdims=True)
    return (values * lax.rsqrt(mean_sq + NORM_EPS) * gain_row).astype(BF16)


def rope_tables(lengths, head_dim):
    inv_freq = ROPE_THETA ** (-jnp.arange(head_dim // 2, dtype=F32) * (2.0 / head_dim))
    angles = lengths.astype(F32)[..., None] * inv_freq
    cos_part, sin_part = jnp.cos(angles), jnp.sin(angles)
    return jnp.concatenate([cos_part, cos_part], -1), jnp.concatenate([-sin_part, sin_part], -1)


def column_chunks(total, width):
    return [(low, min(width, total - low)) for low in range(0, total, width)]


def dot(lhs, rhs):
    return jnp.dot(lhs, rhs, preferred_element_type=F32)


def pipeline_kernel(
    stages, batch, lens_ref, gain_ref, cos_ref, sin_ref, emb_ref, wqkv_hbm, wout_hbm, wgate_hbm, wup_hbm, wdown_hbm, kc_hbm, vc_hbm,
    final_ref, knew_ref, vnew_ref,
    wqkv, wout, wgate, wup, wdown, kbuf, vbuf, xbuf, xout, resid, send_a, recv_a, send_d, recv_d, unit, hidden, attn, q_scr, k_scr, v_scr, o_scr,
    w_sem, c_sem, n_sem, e_sem, a_send, a_recv, d_send, d_recv, x_send, x_recv, f_send, f_recv, credit,
):
    stage = lax.axis_index("stage")
    peer = {"tp": 1 - lax.axis_index("tp")}
    last = stages - 1
    rows = emb_ref.shape[0]
    count = rows // batch
    heads, head_dim = kbuf.shape[2], kbuf.shape[3]
    slots = kbuf.shape[1]
    scale = head_dim ** -0.5
    weights = [pltpu.make_async_copy(src, dst, w_sem.at[i]) for i, (src, dst) in enumerate(
        [(wqkv_hbm, wqkv), (wout_hbm, wout), (wgate_hbm, wgate), (wup_hbm, wup), (wdown_hbm, wdown)])]

    def span(step):
        return pl.ds(pl.multiple_of(step * batch, batch), batch)

    def emb_copy(step):
        return pltpu.make_async_copy(emb_ref.at[span(step)], xbuf.at[lax.rem(step, 2)], e_sem.at[lax.rem(step, 2)])

    def cache_copies(step):
        return (pltpu.make_async_copy(kc_hbm.at[span(step)], kbuf, c_sem.at[0]), pltpu.make_async_copy(vc_hbm.at[span(step)], vbuf, c_sem.at[1]))

    def new_copies(step):
        return (pltpu.make_async_copy(k_scr, knew_ref.at[span(step)], n_sem.at[0]), pltpu.make_async_copy(v_scr, vnew_ref.at[span(step)], n_sem.at[1]))

    def sum_copy(step, send, recv, send_sem, recv_sem):
        slot = lax.rem(step, 2)
        return pltpu.make_async_remote_copy(send.at[slot], recv.at[slot], send_sem.at[slot], recv_sem.at[slot], device_id=peer, device_id_type=MESH)

    def hop_copy(step):
        slot = lax.rem(step, 2)
        return pltpu.make_async_remote_copy(xout.at[slot], xbuf.at[slot], x_send.at[slot], x_recv.at[slot], device_id={"stage": stage + 1}, device_id_type=MESH)

    def final_copies(step):
        slot = lax.rem(step, 2)
        return [pltpu.make_async_remote_copy(xout.at[slot], final_ref.at[span(step)], f_send.at[slot, dst], f_recv.at[step], device_id={"stage": dst}, device_id_type=MESH)
                for dst in range(last)]

    def final_local(step):
        slot = lax.rem(step, 2)
        return pltpu.make_async_copy(xout.at[slot], final_ref.at[span(step)], f_send.at[slot, last])

    for copy in weights[:1] + list(cache_copies(0)) + weights[1:]:
        copy.start()

    @pl.when(stage == 0)
    def _():
        emb_copy(0).start()
        emb_copy(1).start()

    def attend(step):
        slot = lax.rem(step, 2)

        @pl.when(stage == 0)
        def _():
            emb_copy(step).wait()

        @pl.when(stage > 0)
        def _():
            pltpu.make_async_remote_copy(xout.at[slot], xbuf.at[slot], x_send.at[slot], x_recv.at[slot], device_id={"stage": stage}, device_id_type=MESH).wait_recv()

        @pl.when(step == 0)
        def _():
            weights[0].wait()

        @pl.when(step > 0)
        def _():
            for copy in new_copies(step - 1):
                copy.wait()

        unit[...] = rms_norm(xbuf[slot].astype(F32), gain_ref[0:1, :])
        cos_part = cos_ref[span(step), :]
        sin_part = sin_ref[span(step), :]
        for low, width in column_chunks(wqkv.shape[1], 8 * head_dim):
            proj = dot(unit[...], wqkv[:, low:low + width])
            for part in range(width // head_dim):
                kind, head = divmod(low // head_dim + part, heads)
                piece = proj[:, part * head_dim:(part + 1) * head_dim]
                if kind < 2:
                    piece = piece * cos_part + pltpu.roll(piece, head_dim // 2, 1) * sin_part
                (q_scr, k_scr, v_scr)[kind][:, head, :] = piece.astype(BF16).astype(F32)
        for copy in cache_copies(step):
            copy.wait()
        for copy in new_copies(step):
            copy.start()
        used = slots - 1
        position = lax.broadcasted_iota(jnp.int32, (used - MIN_LENGTH, heads, 1), 0) + MIN_LENGTH

        def one_row(row):
            length = lens_ref[step * batch + row]
            query = q_scr[row] * (scale * LOG2_E)
            scores = jnp.sum(query[None] * kbuf[row, :used].astype(F32), axis=-1, keepdims=True)
            scores = jnp.concatenate([scores[:MIN_LENGTH], jnp.where(position < length, scores[MIN_LENGTH:], -jnp.inf)], axis=0)
            fresh = jnp.sum(query * k_scr[row], axis=-1, keepdims=True)
            peak = jnp.maximum(jnp.max(scores, axis=0), fresh)
            exps = jnp.exp2(scores - peak[None])
            fresh_exp = jnp.exp2(fresh - peak)
            inverse = 1.0 / (jnp.sum(exps, axis=0) + fresh_exp)
            probs = (exps * inverse[None]).astype(BF16).astype(F32)
            fresh_prob = (fresh_exp * inverse).astype(BF16).astype(F32)
            o_scr[row] = jnp.sum(probs * vbuf[row, :used].astype(F32), axis=0) + fresh_prob * v_scr[row]

        def rows_body(index, carry):
            for sub in range(ROW_UNROLL):
                one_row(index * ROW_UNROLL + sub)
            return carry

        lax.fori_loop(0, batch // ROW_UNROLL, rows_body, 0)

        @pl.when(step + 1 < count)
        def _():
            for copy in cache_copies(step + 1):
                copy.start()

    def project(step):
        slot = lax.rem(step, 2)

        @pl.when(step == 0)
        def _():
            weights[1].wait()

        for head in range(heads):
            attn[:, head * head_dim:(head + 1) * head_dim] = o_scr[:, head, :].astype(BF16)
        for low, width in column_chunks(wout.shape[1], 1024):
            partial = dot(attn[...], wout[:, low:low + width])
            send_a[slot, :, low:low + width] = partial.astype(BF16)
            resid[slot, :, low:low + width] = xbuf[slot, :, low:low + width].astype(F32) + partial
        sum_copy(step, send_a, recv_a, a_send, a_recv).start()

        @pl.when(jnp.logical_and(stage == 0, step + 2 < count))
        def _():
            emb_copy(step + 2).start()

        @pl.when(jnp.logical_and(stage > 0, step + 2 < count))
        def _():
            pl.semaphore_signal(credit, inc=1, device_id={"stage": stage - 1}, device_id_type=MESH)

    def feed_forward(step):
        slot = lax.rem(step, 2)

        @pl.when(step == 0)
        def _():
            for copy in weights[2:]:
                copy.wait()

        sum_copy(step, send_a, recv_a, a_send, a_recv).wait()
        summed = resid[slot] + recv_a[slot].astype(F32)
        resid[slot] = summed
        unit[...] = rms_norm(summed, gain_ref[1:2, :])
        for low, width in column_chunks(wgate.shape[1], 768):
            gate = dot(unit[...], wgate[:, low:low + width])
            up = dot(unit[...], wup[:, low:low + width])
            hidden[:, low:low + width] = (jax.nn.silu(gate) * up).astype(BF16)
        for low, width in column_chunks(wdown.shape[1], 1024):
            partial = dot(hidden[...], wdown[:, low:low + width])
            send_d[slot, :, low:low + width] = partial.astype(BF16)
            resid[slot, :, low:low + width] = resid[slot, :, low:low + width] + partial
        sum_copy(step, send_d, recv_d, d_send, d_recv).start()

    def hand_on(step):
        slot = lax.rem(step, 2)
        sum_copy(step, send_d, recv_d, d_send, d_recv).wait()

        @pl.when(jnp.logical_and(stage < last, step >= 2))
        def _():
            hop_copy(step - 2).wait_send()
            pl.semaphore_wait(credit, 1)

        @pl.when(jnp.logical_and(stage == last, step >= 2))
        def _():
            for copy in final_copies(step - 2):
                copy.wait_send()
            final_local(step - 2).wait()

        xout[slot] = (resid[slot] + recv_d[slot].astype(F32)).astype(BF16)

        @pl.when(stage < last)
        def _():
            hop_copy(step).start()

        @pl.when(stage == last)
        def _():
            for copy in final_copies(step):
                copy.start()
            final_local(step).start()

    def slot_body(step, carry):
        @pl.when(step < count)
        def _():
            attend(step)

        @pl.when(step >= 2)
        def _():
            hand_on(step - 2)

        @pl.when(step < count)
        def _():
            project(step)

        @pl.when(jnp.logical_and(step >= 1, step <= count))
        def _():
            feed_forward(step - 1)

        return carry

    lax.fori_loop(0, count + 2, slot_body, 0)
    for copy in new_copies(count - 1):
        copy.wait()

    @pl.when(stage < last)
    def _():
        for step in (count - 2, count - 1):
            hop_copy(step).wait_send()

        def drain(step, carry):
            pltpu.make_async_remote_copy(xout.at[0], final_ref.at[span(step)], f_send.at[0, 0], f_recv.at[step], device_id={"stage": stage}, device_id_type=MESH).wait_recv()
            return carry

        lax.fori_loop(0, count, drain, 0)

    @pl.when(stage == last)
    def _():
        for step in (count - 2, count - 1):
            for copy in final_copies(step):
                copy.wait_send()
            final_local(step).wait()


def run_pipeline(stages, lens, gains, cos_part, sin_part, embeds, wqkv, wout, wgate, wup, wdown, k_cache, v_cache):
    rows, width = embeds.shape
    batch = 16 * MERGE
    slots, heads, head_dim = k_cache.shape[1:]
    count = rows // batch
    anywhere = pl.BlockSpec(memory_space=pl.ANY)
    local = pl.BlockSpec(memory_space=pltpu.VMEM)
    pair = pltpu.SemaphoreType.DMA((2,))
    new_rows = jax.ShapeDtypeStruct((rows, heads, head_dim), F32)
    return pl.pallas_call(
        functools.partial(pipeline_kernel, stages, batch),
        out_shape=(jax.ShapeDtypeStruct((rows, width), BF16), new_rows, new_rows),
        in_specs=[pl.BlockSpec(memory_space=pltpu.SMEM), local, local, local] + [anywhere] * 8,
        out_specs=(anywhere, anywhere, anywhere),
        scratch_shapes=[
            pltpu.VMEM(wqkv.shape, BF16), pltpu.VMEM(wout.shape, BF16), pltpu.VMEM(wgate.shape, BF16), pltpu.VMEM(wup.shape, BF16), pltpu.VMEM(wdown.shape, BF16),
            pltpu.VMEM((batch, slots, heads, head_dim), BF16), pltpu.VMEM((batch, slots, heads, head_dim), BF16),
            pltpu.VMEM((2, batch, width), BF16), pltpu.VMEM((2, batch, width), BF16), pltpu.VMEM((2, batch, width), F32),
            pltpu.VMEM((2, batch, width), BF16), pltpu.VMEM((2, batch, width), BF16), pltpu.VMEM((2, batch, width), BF16), pltpu.VMEM((2, batch, width), BF16),
            pltpu.VMEM((batch, width), BF16), pltpu.VMEM((batch, wgate.shape[1]), BF16), pltpu.VMEM((batch, heads * head_dim), BF16),
            pltpu.VMEM((batch, heads, head_dim), F32), pltpu.VMEM((batch, heads, head_dim), F32), pltpu.VMEM((batch, heads, head_dim), F32), pltpu.VMEM((batch, heads, head_dim), F32),
            pltpu.SemaphoreType.DMA((5,)), pair, pair, pair, pair, pair, pair, pair, pair, pair,
            pltpu.SemaphoreType.DMA((2, stages)), pltpu.SemaphoreType.DMA((count,)), pltpu.SemaphoreType.REGULAR,
        ],
        compiler_params=pltpu.CompilerParams(has_side_effects=True, vmem_limit_bytes=VMEM_LIMIT),
    )(lens, gains, cos_part, sin_part, embeds, wqkv, wout, wgate, wup, wdown, k_cache, v_cache)


def tail_kernel(lens_ref, gain_ref, final_ref, knew_ref, vnew_ref, kc_ref, vc_ref, wun_ref, logits_ref, ko_ref, vo_ref, normed):
    block = pl.program_id(0)
    rows = kc_ref.shape[0]

    @pl.when(block == 0)
    def _():
        normed[...] = rms_norm(final_ref[...].astype(F32), gain_ref[...])

    ko_ref[...] = kc_ref[...]
    vo_ref[...] = vc_ref[...]

    def place(row, carry):
        length = lens_ref[block * rows + row]
        ko_ref[row, length] = knew_ref[row].astype(BF16)
        vo_ref[row, length] = vnew_ref[row].astype(BF16)
        return carry

    lax.fori_loop(0, rows, place, 0)
    logits_ref[...] = lax.dot_general(normed[...], wun_ref[...], (((1,), (1,)), ((), ())), preferred_element_type=F32)


def run_tail(lens, gain, final, knew, vnew, k_cache, v_cache, wun):
    rows, width = final.shape
    slots, heads, head_dim = k_cache.shape[1:]
    vocab = wun.shape[0]
    block = rows // TAIL_STEPS
    columns = pl.cdiv(vocab, TAIL_STEPS * 128) * 128
    cache_spec = pl.BlockSpec((block, slots, heads, head_dim), lambda i, lens: (i, 0, 0, 0))
    new_spec = pl.BlockSpec((block, heads, head_dim), lambda i, lens: (i, 0, 0))
    return pl.pallas_call(
        tail_kernel,
        out_shape=(jax.ShapeDtypeStruct((rows, vocab), F32), jax.ShapeDtypeStruct(k_cache.shape, BF16), jax.ShapeDtypeStruct(v_cache.shape, BF16)),
        grid_spec=pltpu.PrefetchScalarGridSpec(
            num_scalar_prefetch=1,
            grid=(TAIL_STEPS,),
            in_specs=[pl.BlockSpec((1, width), lambda i, lens: (0, 0)), pl.BlockSpec((rows, width), lambda i, lens: (0, 0)), new_spec, new_spec, cache_spec, cache_spec,
                      pl.BlockSpec((columns, width), lambda i, lens: (i, 0))],
            out_specs=(pl.BlockSpec((rows, columns), lambda i, lens: (0, i)), cache_spec, cache_spec),
            scratch_shapes=[pltpu.VMEM((rows, width), BF16)],
        ),
        compiler_params=pltpu.CompilerParams(dimension_semantics=("arbitrary",), vmem_limit_bytes=VMEM_LIMIT),
    )(lens, gain, final, knew, vnew, k_cache, v_cache, wun)


def solution(mesh):
    stages = mesh.shape['stage']
    cache_spec = P('stage', 'replica', None, None, 'tp', None)
    in_specs = (P('replica'), P('stage', None, 'tp', None, None), P('stage', 'tp', None), P('stage', None, 'tp'), P('stage', None, 'tp'), P('stage', 'tp', None), P('stage'), cache_spec, cache_spec, P('replica'), P(), P(None, ('stage', 'tp')))
    out_specs = (P('replica', None, ('stage', 'tp')), cache_spec, cache_spec)

    def device_step(embeds, w_qkv, w_out, w_gate, w_up, w_down, norm_gain, k_cache, v_cache, lengths, final_gain, w_unembed):
        groups, seqs, width = embeds.shape
        rows = groups * seqs
        cache_shape = k_cache.shape
        head_dim = cache_shape[-1]
        lens = lengths.reshape(rows)
        cos_part, sin_part = rope_tables(lens, head_dim)
        k_rows = k_cache.reshape((rows,) + cache_shape[3:])
        v_rows = v_cache.reshape((rows,) + cache_shape[3:])
        final, knew, vnew = run_pipeline(
            stages, lens, norm_gain[0], cos_part, sin_part, embeds.reshape(rows, width), w_qkv[0].transpose(0, 2, 1, 3).reshape(width, -1), w_out[0], w_gate[0], w_up[0], w_down[0], k_rows, v_rows)
        logits, k_out, v_out = run_tail(lens, final_gain.reshape(1, width), final, knew, vnew, k_rows, v_rows, w_unembed.T)
        return logits.reshape(groups, seqs, -1), k_out.reshape(cache_shape), v_out.reshape(cache_shape)

    return jax.shard_map(device_step, mesh=mesh, in_specs=in_specs, out_specs=out_specs, check_vma=False)
```

```python
import functools

import jax
import jax.numpy as jnp
from jax import lax
from jax.experimental import pallas as pl
from jax.experimental.pallas import tpu as pltpu
from jax.sharding import PartitionSpec as P

NORM_EPS = 1e-5
ROPE_THETA = 10000.0
MESH = pl.DeviceIdType.MESH
F32 = jnp.float32
BF16 = jnp.bfloat16
MERGE = 4
TAIL_STEPS = 16
LOG2_E = 1.4426950408889634
ROW_UNROLL = 16
VMEM_LIMIT = 67043328


def rms_norm(values, gain_row):
    mean_sq = jnp.mean(values * values, axis=-1, keepdims=True)
    return (values * lax.rsqrt(mean_sq + NORM_EPS) * gain_row).astype(BF16)


def rope_tables(lengths, head_dim):
    inv_freq = ROPE_THETA ** (-jnp.arange(head_dim // 2, dtype=F32) * (2.0 / head_dim))
    angles = lengths.astype(F32)[..., None] * inv_freq
    cos_part, sin_part = jnp.cos(angles), jnp.sin(angles)
    return jnp.concatenate([cos_part, cos_part], -1), jnp.concatenate([-sin_part, sin_part], -1)


def column_chunks(total, width):
    return [(low, min(width, total - low)) for low in range(0, total, width)]


def dot(lhs, rhs):
    return jnp.dot(lhs, rhs, preferred_element_type=F32)


def pipeline_kernel(
    stages, batch, lens_ref, gain_ref, cos_ref, sin_ref, emb_ref, wqkv_hbm, wout_hbm, wgate_hbm, wup_hbm, wdown_hbm, kc_hbm, vc_hbm,
    final_ref, knew_ref, vnew_ref,
    wqkv, wout, wgate, wup, wdown, kbuf, vbuf, xbuf, xout, resid, send_a, recv_a, send_d, recv_d, unit, hidden, attn, q_scr, k_scr, v_scr, o_scr,
    w_sem, c_sem, n_sem, e_sem, a_send, a_recv, d_send, d_recv, x_send, x_recv, f_send, f_recv, credit,
):
    stage = lax.axis_index("stage")
    peer = {"tp": 1 - lax.axis_index("tp")}
    last = stages - 1
    rows = emb_ref.shape[0]
    count = rows // batch
    heads, head_dim = kbuf.shape[2], kbuf.shape[3]
    slots = kbuf.shape[1]
    scale = head_dim ** -0.5
    weights = [pltpu.make_async_copy(src, dst, w_sem.at[i]) for i, (src, dst) in enumerate(
        [(wqkv_hbm, wqkv), (wout_hbm, wout), (wgate_hbm, wgate), (wup_hbm, wup), (wdown_hbm, wdown)])]

    def span(step):
        return pl.ds(pl.multiple_of(step * batch, batch), batch)

    def emb_copy(step):
        return pltpu.make_async_copy(emb_ref.at[span(step)], xbuf.at[lax.rem(step, 2)], e_sem.at[lax.rem(step, 2)])

    def cache_copies(step):
        return (pltpu.make_async_copy(kc_hbm.at[span(step)], kbuf, c_sem.at[0]), pltpu.make_async_copy(vc_hbm.at[span(step)], vbuf, c_sem.at[1]))

    def new_copies(step):
        return (pltpu.make_async_copy(k_scr, knew_ref.at[span(step)], n_sem.at[0]), pltpu.make_async_copy(v_scr, vnew_ref.at[span(step)], n_sem.at[1]))

    def sum_copy(step, send, recv, send_sem, recv_sem):
        slot = lax.rem(step, 2)
        return pltpu.make_async_remote_copy(send.at[slot], recv.at[slot], send_sem.at[slot], recv_sem.at[slot], device_id=peer, device_id_type=MESH)

    def hop_copy(step):
        slot = lax.rem(step, 2)
        return pltpu.make_async_remote_copy(xout.at[slot], xbuf.at[slot], x_send.at[slot], x_recv.at[slot], device_id={"stage": stage + 1}, device_id_type=MESH)

    def final_copies(step):
        slot = lax.rem(step, 2)
        return [pltpu.make_async_remote_copy(xout.at[slot], final_ref.at[span(step)], f_send.at[slot, dst], f_recv.at[step], device_id={"stage": dst}, device_id_type=MESH)
                for dst in range(last)]

    def final_local(step):
        slot = lax.rem(step, 2)
        return pltpu.make_async_copy(xout.at[slot], final_ref.at[span(step)], f_send.at[slot, last])

    for copy in weights[:1] + list(cache_copies(0)) + weights[1:]:
        copy.start()

    @pl.when(stage == 0)
    def _():
        emb_copy(0).start()
        emb_copy(1).start()

    def attend(step):
        slot = lax.rem(step, 2)

        @pl.when(stage == 0)
        def _():
            emb_copy(step).wait()

        @pl.when(stage > 0)
        def _():
            pltpu.make_async_remote_copy(xout.at[slot], xbuf.at[slot], x_send.at[slot], x_recv.at[slot], device_id={"stage": stage}, device_id_type=MESH).wait_recv()

        @pl.when(step == 0)
        def _():
            weights[0].wait()

        @pl.when(step > 0)
        def _():
            for copy in new_copies(step - 1):
                copy.wait()

        unit[...] = rms_norm(xbuf[slot].astype(F32), gain_ref[0:1, :])
        cos_part = cos_ref[span(step), :]
        sin_part = sin_ref[span(step), :]
        for low, width in column_chunks(wqkv.shape[1], 8 * head_dim):
            proj = dot(unit[...], wqkv[:, low:low + width])
            for part in range(width // head_dim):
                kind, head = divmod(low // head_dim + part, heads)
                piece = proj[:, part * head_dim:(part + 1) * head_dim]
                if kind < 2:
                    piece = piece * cos_part + pltpu.roll(piece, head_dim // 2, 1) * sin_part
                (q_scr, k_scr, v_scr)[kind][:, head, :] = piece.astype(BF16).astype(F32)
        for copy in cache_copies(step):
            copy.wait()
        for copy in new_copies(step):
            copy.start()
        used = slots - 1
        lane = lax.broadcasted_iota(jnp.int32, (heads, head_dim), 1)

        def score_rows(index, carry):
            group = pl.ds(index * ROW_UNROLL, ROW_UNROLL)
            query = q_scr[group] * (scale * LOG2_E)
            packed = jnp.where(lane == used, jnp.sum(query * k_scr[group], axis=-1, keepdims=True), -jnp.inf)
            for slot_idx in range(used):
                packed = jnp.where(lane == slot_idx, jnp.sum(query * kbuf[group, slot_idx].astype(F32), axis=-1, keepdims=True), packed)
            for sub in range(ROW_UNROLL):
                length = lens_ref[step * batch + index * ROW_UNROLL + sub]
                q_scr[index * ROW_UNROLL + sub] = jnp.where(jnp.logical_or(lane < length, lane == used), packed[sub], -jnp.inf)
            return carry

        lax.fori_loop(0, batch // ROW_UNROLL, score_rows, 0)
        packed = q_scr[...]
        exps = jnp.exp2(packed - jnp.max(packed, axis=-1, keepdims=True))
        q_scr[...] = (exps * (1.0 / jnp.sum(exps, axis=-1, keepdims=True))).astype(BF16).astype(F32)

        def value_rows(index, carry):
            group = pl.ds(index * ROW_UNROLL, ROW_UNROLL)
            probs = q_scr[group]
            total = probs[:, :, used:used + 1] * v_scr[group]
            for slot_idx in range(used):
                total = total + probs[:, :, slot_idx:slot_idx + 1] * vbuf[group, slot_idx].astype(F32)
            o_scr[group] = total
            return carry

        lax.fori_loop(0, batch // ROW_UNROLL, value_rows, 0)

        @pl.when(step + 1 < count)
        def _():
            for copy in cache_copies(step + 1):
                copy.start()

    def project(step):
        slot = lax.rem(step, 2)

        @pl.when(step == 0)
        def _():
            weights[1].wait()

        for head in range(heads):
            attn[:, head * head_dim:(head + 1) * head_dim] = o_scr[:, head, :].astype(BF16)
        for low, width in column_chunks(wout.shape[1], 1024):
            partial = dot(attn[...], wout[:, low:low + width])
            send_a[slot, :, low:low + width] = partial.astype(BF16)
            resid[slot, :, low:low + width] = xbuf[slot, :, low:low + width].astype(F32) + partial
        sum_copy(step, send_a, recv_a, a_send, a_recv).start()

        @pl.when(jnp.logical_and(stage == 0, step + 2 < count))
        def _():
            emb_copy(step + 2).start()

        @pl.when(jnp.logical_and(stage > 0, step + 2 < count))
        def _():
            pl.semaphore_signal(credit, inc=1, device_id={"stage": stage - 1}, device_id_type=MESH)

    def feed_forward(step):
        slot = lax.rem(step, 2)

        @pl.when(step == 0)
        def _():
            for copy in weights[2:]:
                copy.wait()

        sum_copy(step, send_a, recv_a, a_send, a_recv).wait()
        summed = resid[slot] + recv_a[slot].astype(F32)
        resid[slot] = summed
        unit[...] = rms_norm(summed, gain_ref[1:2, :])
        for low, width in column_chunks(wgate.shape[1], 768):
            gate = dot(unit[...], wgate[:, low:low + width])
            up = dot(unit[...], wup[:, low:low + width])
            hidden[:, low:low + width] = (jax.nn.silu(gate) * up).astype(BF16)
        for low, width in column_chunks(wdown.shape[1], 1024):
            partial = dot(hidden[...], wdown[:, low:low + width])
            send_d[slot, :, low:low + width] = partial.astype(BF16)
            resid[slot, :, low:low + width] = resid[slot, :, low:low + width] + partial
        sum_copy(step, send_d, recv_d, d_send, d_recv).start()

    def hand_on(step):
        slot = lax.rem(step, 2)
        sum_copy(step, send_d, recv_d, d_send, d_recv).wait()

        @pl.when(jnp.logical_and(stage < last, step >= 2))
        def _():
            hop_copy(step - 2).wait_send()
            pl.semaphore_wait(credit, 1)

        @pl.when(jnp.logical_and(stage == last, step >= 2))
        def _():
            for copy in final_copies(step - 2):
                copy.wait_send()
            final_local(step - 2).wait()

        xout[slot] = (resid[slot] + recv_d[slot].astype(F32)).astype(BF16)

        @pl.when(stage < last)
        def _():
            hop_copy(step).start()

        @pl.when(stage == last)
        def _():
            for copy in final_copies(step):
                copy.start()
            final_local(step).start()

    def slot_body(step, carry):
        @pl.when(step < count)
        def _():
            attend(step)

        @pl.when(step >= 2)
        def _():
            hand_on(step - 2)

        @pl.when(step < count)
        def _():
            project(step)

        @pl.when(jnp.logical_and(step >= 1, step <= count))
        def _():
            feed_forward(step - 1)

        return carry

    lax.fori_loop(0, count + 2, slot_body, 0)
    for copy in new_copies(count - 1):
        copy.wait()

    @pl.when(stage < last)
    def _():
        for step in (count - 2, count - 1):
            hop_copy(step).wait_send()

        def drain(step, carry):
            pltpu.make_async_remote_copy(xout.at[0], final_ref.at[span(step)], f_send.at[0, 0], f_recv.at[step], device_id={"stage": stage}, device_id_type=MESH).wait_recv()
            return carry

        lax.fori_loop(0, count, drain, 0)

    @pl.when(stage == last)
    def _():
        for step in (count - 2, count - 1):
            for copy in final_copies(step):
                copy.wait_send()
            final_local(step).wait()


def run_pipeline(stages, lens, gains, cos_part, sin_part, embeds, wqkv, wout, wgate, wup, wdown, k_cache, v_cache):
    rows, width = embeds.shape
    batch = 16 * MERGE
    slots, heads, head_dim = k_cache.shape[1:]
    count = rows // batch
    anywhere = pl.BlockSpec(memory_space=pl.ANY)
    local = pl.BlockSpec(memory_space=pltpu.VMEM)
    pair = pltpu.SemaphoreType.DMA((2,))
    new_rows = jax.ShapeDtypeStruct((rows, heads, head_dim), F32)
    return pl.pallas_call(
        functools.partial(pipeline_kernel, stages, batch),
        out_shape=(jax.ShapeDtypeStruct((rows, width), BF16), new_rows, new_rows),
        in_specs=[pl.BlockSpec(memory_space=pltpu.SMEM), local, local, local] + [anywhere] * 8,
        out_specs=(anywhere, anywhere, anywhere),
        scratch_shapes=[
            pltpu.VMEM(wqkv.shape, BF16), pltpu.VMEM(wout.shape, BF16), pltpu.VMEM(wgate.shape, BF16), pltpu.VMEM(wup.shape, BF16), pltpu.VMEM(wdown.shape, BF16),
            pltpu.VMEM((batch, slots, heads, head_dim), BF16), pltpu.VMEM((batch, slots, heads, head_dim), BF16),
            pltpu.VMEM((2, batch, width), BF16), pltpu.VMEM((2, batch, width), BF16), pltpu.VMEM((2, batch, width), F32),
            pltpu.VMEM((2, batch, width), BF16), pltpu.VMEM((2, batch, width), BF16), pltpu.VMEM((2, batch, width), BF16), pltpu.VMEM((2, batch, width), BF16),
            pltpu.VMEM((batch, width), BF16), pltpu.VMEM((batch, wgate.shape[1]), BF16), pltpu.VMEM((batch, heads * head_dim), BF16),
            pltpu.VMEM((batch, heads, head_dim), F32), pltpu.VMEM((batch, heads, head_dim), F32), pltpu.VMEM((batch, heads, head_dim), F32), pltpu.VMEM((batch, heads, head_dim), F32),
            pltpu.SemaphoreType.DMA((5,)), pair, pair, pair, pair, pair, pair, pair, pair, pair,
            pltpu.SemaphoreType.DMA((2, stages)), pltpu.SemaphoreType.DMA((count,)), pltpu.SemaphoreType.REGULAR,
        ],
        compiler_params=pltpu.CompilerParams(has_side_effects=True, vmem_limit_bytes=VMEM_LIMIT),
    )(lens, gains, cos_part, sin_part, embeds, wqkv, wout, wgate, wup, wdown, k_cache, v_cache)


def tail_kernel(lens_ref, gain_ref, final_ref, knew_ref, vnew_ref, kc_ref, vc_ref, wun_ref, logits_ref, ko_ref, vo_ref, normed):
    block = pl.program_id(0)
    rows = kc_ref.shape[0]

    @pl.when(block == 0)
    def _():
        normed[...] = rms_norm(final_ref[...].astype(F32), gain_ref[...])

    ko_ref[...] = kc_ref[...]
    vo_ref[...] = vc_ref[...]

    def place(row, carry):
        length = lens_ref[block * rows + row]
        ko_ref[row, length] = knew_ref[row].astype(BF16)
        vo_ref[row, length] = vnew_ref[row].astype(BF16)
        return carry

    lax.fori_loop(0, rows, place, 0)
    logits_ref[...] = lax.dot_general(normed[...], wun_ref[...], (((1,), (1,)), ((), ())), preferred_element_type=F32)


def run_tail(lens, gain, final, knew, vnew, k_cache, v_cache, wun):
    rows, width = final.shape
    slots, heads, head_dim = k_cache.shape[1:]
    vocab = wun.shape[0]
    block = rows // TAIL_STEPS
    columns = pl.cdiv(vocab, TAIL_STEPS * 128) * 128
    cache_spec = pl.BlockSpec((block, slots, heads, head_dim), lambda i, lens: (i, 0, 0, 0))
    new_spec = pl.BlockSpec((block, heads, head_dim), lambda i, lens: (i, 0, 0))
    return pl.pallas_call(
        tail_kernel,
        out_shape=(jax.ShapeDtypeStruct((rows, vocab), F32), jax.ShapeDtypeStruct(k_cache.shape, BF16), jax.ShapeDtypeStruct(v_cache.shape, BF16)),
        grid_spec=pltpu.PrefetchScalarGridSpec(
            num_scalar_prefetch=1,
            grid=(TAIL_STEPS,),
            in_specs=[pl.BlockSpec((1, width), lambda i, lens: (0, 0)), pl.BlockSpec((rows, width), lambda i, lens: (0, 0)), new_spec, new_spec, cache_spec, cache_spec,
                      pl.BlockSpec((columns, width), lambda i, lens: (i, 0))],
            out_specs=(pl.BlockSpec((rows, columns), lambda i, lens: (0, i)), cache_spec, cache_spec),
            scratch_shapes=[pltpu.VMEM((rows, width), BF16)],
        ),
        compiler_params=pltpu.CompilerParams(dimension_semantics=("arbitrary",), vmem_limit_bytes=VMEM_LIMIT),
    )(lens, gain, final, knew, vnew, k_cache, v_cache, wun)


def solution(mesh):
    stages = mesh.shape['stage']
    cache_spec = P('stage', 'replica', None, None, 'tp', None)
    in_specs = (P('replica'), P('stage', None, 'tp', None, None), P('stage', 'tp', None), P('stage', None, 'tp'), P('stage', None, 'tp'), P('stage', 'tp', None), P('stage'), cache_spec, cache_spec, P('replica'), P(), P(None, ('stage', 'tp')))
    out_specs = (P('replica', None, ('stage', 'tp')), cache_spec, cache_spec)

    def device_step(embeds, w_qkv, w_out, w_gate, w_up, w_down, norm_gain, k_cache, v_cache, lengths, final_gain, w_unembed):
        groups, seqs, width = embeds.shape
        rows = groups * seqs
        cache_shape = k_cache.shape
        head_dim = cache_shape[-1]
        lens = lengths.reshape(rows)
        cos_part, sin_part = rope_tables(lens, head_dim)
        k_rows = k_cache.reshape((rows,) + cache_shape[3:])
        v_rows = v_cache.reshape((rows,) + cache_shape[3:])
        final, knew, vnew = run_pipeline(
            stages, lens, norm_gain[0], cos_part, sin_part, embeds.reshape(rows, width), w_qkv[0].transpose(0, 2, 1, 3).reshape(width, -1), w_out[0], w_gate[0], w_up[0], w_down[0], k_rows, v_rows)
        logits, k_out, v_out = run_tail(lens, final_gain.reshape(1, width), final, knew, vnew, k_rows, v_rows, w_unembed.T)
        return logits.reshape(groups, seqs, -1), k_out.reshape(cache_shape), v_out.reshape(cache_shape)

    return jax.shard_map(device_step, mesh=mesh, in_specs=in_specs, out_specs=out_specs, check_vma=False)
```

```python
import functools

import jax
import jax.numpy as jnp
from jax import lax
from jax.experimental import pallas as pl
from jax.experimental.pallas import tpu as pltpu
from jax.sharding import PartitionSpec as P

NORM_EPS = 1e-5
ROPE_THETA = 10000.0
MESH = pl.DeviceIdType.MESH
F32 = jnp.float32
BF16 = jnp.bfloat16
MERGE = 4
TAIL_STEPS = 16
LOG2_E = 1.4426950408889634
ROW_UNROLL = 16
CHUNKS = 2
VMEM_LIMIT = 67043328


def rms_norm(values, gain_row):
    mean_sq = jnp.mean(values * values, axis=-1, keepdims=True)
    return (values * lax.rsqrt(mean_sq + NORM_EPS) * gain_row).astype(BF16)


def rope_tables(lengths, head_dim):
    inv_freq = ROPE_THETA ** (-jnp.arange(head_dim // 2, dtype=F32) * (2.0 / head_dim))
    angles = lengths.astype(F32)[..., None] * inv_freq
    cos_part, sin_part = jnp.cos(angles), jnp.sin(angles)
    return jnp.concatenate([cos_part, cos_part], -1), jnp.concatenate([-sin_part, sin_part], -1)


def column_chunks(total, width):
    return [(low, min(width, total - low)) for low in range(0, total, width)]


def joined(ref, slot):
    return jnp.concatenate([ref[slot, chunk].astype(F32) for chunk in range(CHUNKS)], axis=-1)


def dot(lhs, rhs):
    return jnp.dot(lhs, rhs, preferred_element_type=F32)


def pipeline_kernel(
    stages, batch, lens_ref, gain_ref, cos_ref, sin_ref, emb_ref, wqkv_hbm, wout_hbm, wgate_hbm, wup_hbm, wdown_hbm, kc_hbm, vc_hbm,
    final_ref, knew_ref, vnew_ref,
    wqkv, wout, wgate, wup, wdown, kbuf, vbuf, xbuf, xout, resid, send_a, recv_a, send_d, recv_d, unit, hidden, attn, q_scr, k_scr, v_scr, o_scr,
    w_sem, c_sem, n_sem, e_sem, a_send, a_recv, d_send, d_recv, x_send, x_recv, f_send, f_recv, credit,
):
    stage = lax.axis_index("stage")
    peer = {"tp": 1 - lax.axis_index("tp")}
    last = stages - 1
    rows = emb_ref.shape[0]
    count = rows // batch
    heads, head_dim = kbuf.shape[2], kbuf.shape[3]
    slots = kbuf.shape[1]
    scale = head_dim ** -0.5
    weights = [pltpu.make_async_copy(src, dst, w_sem.at[i]) for i, (src, dst) in enumerate(
        [(wqkv_hbm, wqkv), (wout_hbm, wout), (wgate_hbm, wgate), (wup_hbm, wup), (wdown_hbm, wdown)])]

    def span(step):
        return pl.ds(pl.multiple_of(step * batch, batch), batch)

    def emb_copy(step):
        return pltpu.make_async_copy(emb_ref.at[span(step)], xbuf.at[lax.rem(step, 2)], e_sem.at[lax.rem(step, 2)])

    def cache_copies(step):
        return (pltpu.make_async_copy(kc_hbm.at[span(step)], kbuf, c_sem.at[0]), pltpu.make_async_copy(vc_hbm.at[span(step)], vbuf, c_sem.at[1]))

    def new_copies(step):
        return (pltpu.make_async_copy(k_scr, knew_ref.at[span(step)], n_sem.at[0]), pltpu.make_async_copy(v_scr, vnew_ref.at[span(step)], n_sem.at[1]))

    def sum_copy(step, chunk, send, recv, send_sem, recv_sem):
        out, into = lax.rem(step, 2), lax.rem(step, 3)
        return pltpu.make_async_remote_copy(send.at[out, chunk], recv.at[into, chunk], send_sem.at[out, chunk], recv_sem.at[into, chunk], device_id=peer, device_id_type=MESH)

    def hop_copy(step):
        slot = lax.rem(step, 2)
        return pltpu.make_async_remote_copy(xout.at[slot], xbuf.at[slot], x_send.at[slot], x_recv.at[slot], device_id={"stage": stage + 1}, device_id_type=MESH)

    def final_copies(step):
        slot = lax.rem(step, 2)
        return [pltpu.make_async_remote_copy(xout.at[slot], final_ref.at[span(step)], f_send.at[slot, dst], f_recv.at[step], device_id={"stage": dst}, device_id_type=MESH)
                for dst in range(last)]

    def final_local(step):
        slot = lax.rem(step, 2)
        return pltpu.make_async_copy(xout.at[slot], final_ref.at[span(step)], f_send.at[slot, last])

    for copy in weights[:1] + list(cache_copies(0)) + weights[1:]:
        copy.start()

    @pl.when(stage == 0)
    def _():
        emb_copy(0).start()
        emb_copy(1).start()

    def attend(step):
        slot = lax.rem(step, 2)

        @pl.when(stage == 0)
        def _():
            emb_copy(step).wait()

        @pl.when(stage > 0)
        def _():
            pltpu.make_async_remote_copy(xout.at[slot], xbuf.at[slot], x_send.at[slot], x_recv.at[slot], device_id={"stage": stage}, device_id_type=MESH).wait_recv()

        @pl.when(step == 0)
        def _():
            weights[0].wait()

        @pl.when(step > 0)
        def _():
            for copy in new_copies(step - 1):
                copy.wait()

        unit[...] = rms_norm(xbuf[slot].astype(F32), gain_ref[0:1, :])
        cos_part = cos_ref[span(step), :]
        sin_part = sin_ref[span(step), :]
        for low, width in column_chunks(wqkv.shape[1], 8 * head_dim):
            proj = dot(unit[...], wqkv[:, low:low + width])
            for part in range(width // head_dim):
                kind, head = divmod(low // head_dim + part, heads)
                piece = proj[:, part * head_dim:(part + 1) * head_dim]
                if kind < 2:
                    piece = piece * cos_part + pltpu.roll(piece, head_dim // 2, 1) * sin_part
                (q_scr, k_scr, v_scr)[kind][:, head, :] = piece.astype(BF16).astype(F32)
        for copy in cache_copies(step):
            copy.wait()
        for copy in new_copies(step):
            copy.start()
        used = slots - 1
        lane = lax.broadcasted_iota(jnp.int32, (heads, head_dim), 1)

        def score_rows(index, carry):
            group = pl.ds(index * ROW_UNROLL, ROW_UNROLL)
            query = q_scr[group] * (scale * LOG2_E)
            packed = jnp.where(lane == used, jnp.sum(query * k_scr[group], axis=-1, keepdims=True), -jnp.inf)
            for slot_idx in range(used):
                packed = jnp.where(lane == slot_idx, jnp.sum(query * kbuf[group, slot_idx].astype(F32), axis=-1, keepdims=True), packed)
            for sub in range(ROW_UNROLL):
                length = lens_ref[step * batch + index * ROW_UNROLL + sub]
                q_scr[index * ROW_UNROLL + sub] = jnp.where(jnp.logical_or(lane < length, lane == used), packed[sub], -jnp.inf)
            return carry

        lax.fori_loop(0, batch // ROW_UNROLL, score_rows, 0)
        packed = q_scr[...]
        exps = jnp.exp2(packed - jnp.max(packed, axis=-1, keepdims=True))
        q_scr[...] = (exps * (1.0 / jnp.sum(exps, axis=-1, keepdims=True))).astype(BF16).astype(F32)

        def value_rows(index, carry):
            group = pl.ds(index * ROW_UNROLL, ROW_UNROLL)
            probs = q_scr[group]
            total = probs[:, :, used:used + 1] * v_scr[group]
            for slot_idx in range(used):
                total = total + probs[:, :, slot_idx:slot_idx + 1] * vbuf[group, slot_idx].astype(F32)
            o_scr[group] = total
            return carry

        lax.fori_loop(0, batch // ROW_UNROLL, value_rows, 0)

        @pl.when(step + 1 < count)
        def _():
            for copy in cache_copies(step + 1):
                copy.start()

    def project(step):
        slot = lax.rem(step, 2)

        @pl.when(step == 0)
        def _():
            weights[1].wait()

        for head in range(heads):
            attn[:, head * head_dim:(head + 1) * head_dim] = o_scr[:, head, :].astype(BF16)
        for chunk, (low, width) in enumerate(column_chunks(wout.shape[1], wout.shape[1] // CHUNKS)):
            partial = dot(attn[...], wout[:, low:low + width])
            send_a[slot, chunk] = partial.astype(BF16)
            resid[lax.rem(step, 3), :, low:low + width] = xbuf[slot, :, low:low + width].astype(F32) + partial
            sum_copy(step, chunk, send_a, recv_a, a_send, a_recv).start()

        @pl.when(jnp.logical_and(stage == 0, step + 2 < count))
        def _():
            emb_copy(step + 2).start()

        @pl.when(jnp.logical_and(stage > 0, step + 2 < count))
        def _():
            pl.semaphore_signal(credit, inc=1, device_id={"stage": stage - 1}, device_id_type=MESH)

    def feed_forward(step):
        slot = lax.rem(step, 2)

        @pl.when(step == 0)
        def _():
            for copy in weights[2:]:
                copy.wait()

        kept = lax.rem(step, 3)
        for chunk in range(CHUNKS):
            sum_copy(step, chunk, send_a, recv_a, a_send, a_recv).wait()
        summed = resid[kept] + joined(recv_a, kept)
        resid[kept] = summed
        unit[...] = rms_norm(summed, gain_ref[1:2, :])
        for low, width in column_chunks(wgate.shape[1], 768):
            gate = dot(unit[...], wgate[:, low:low + width])
            up = dot(unit[...], wup[:, low:low + width])
            hidden[:, low:low + width] = (jax.nn.silu(gate) * up).astype(BF16)
        for chunk, (low, width) in enumerate(column_chunks(wdown.shape[1], wdown.shape[1] // CHUNKS)):
            partial = dot(hidden[...], wdown[:, low:low + width])
            send_d[slot, chunk] = partial.astype(BF16)
            resid[kept, :, low:low + width] = resid[kept, :, low:low + width] + partial
            sum_copy(step, chunk, send_d, recv_d, d_send, d_recv).start()

    def hand_on(step):
        slot = lax.rem(step, 2)
        for chunk in range(CHUNKS):
            sum_copy(step, chunk, send_d, recv_d, d_send, d_recv).wait()

        @pl.when(jnp.logical_and(stage < last, step >= 2))
        def _():
            hop_copy(step - 2).wait_send()
            pl.semaphore_wait(credit, 1)

        @pl.when(jnp.logical_and(stage == last, step >= 2))
        def _():
            for copy in final_copies(step - 2):
                copy.wait_send()
            final_local(step - 2).wait()

        kept = lax.rem(step, 3)
        xout[slot] = (resid[kept] + joined(recv_d, kept)).astype(BF16)

        @pl.when(stage < last)
        def _():
            hop_copy(step).start()

        @pl.when(stage == last)
        def _():
            for copy in final_copies(step):
                copy.start()
            final_local(step).start()

    def slot_body(step, carry):
        @pl.when(step < count)
        def _():
            attend(step)

        @pl.when(step < count)
        def _():
            project(step)

        @pl.when(step >= 2)
        def _():
            hand_on(step - 2)

        @pl.when(jnp.logical_and(step >= 1, step <= count))
        def _():
            feed_forward(step - 1)

        return carry

    lax.fori_loop(0, count + 2, slot_body, 0)
    for copy in new_copies(count - 1):
        copy.wait()

    @pl.when(stage < last)
    def _():
        for step in (count - 2, count - 1):
            hop_copy(step).wait_send()

        def drain(step, carry):
            pltpu.make_async_remote_copy(xout.at[0], final_ref.at[span(step)], f_send.at[0, 0], f_recv.at[step], device_id={"stage": stage}, device_id_type=MESH).wait_recv()
            return carry

        lax.fori_loop(0, count, drain, 0)

    @pl.when(stage == last)
    def _():
        for step in (count - 2, count - 1):
            for copy in final_copies(step):
                copy.wait_send()
            final_local(step).wait()


def run_pipeline(stages, lens, gains, cos_part, sin_part, embeds, wqkv, wout, wgate, wup, wdown, k_cache, v_cache):
    rows, width = embeds.shape
    batch = 16 * MERGE
    slots, heads, head_dim = k_cache.shape[1:]
    count = rows // batch
    anywhere = pl.BlockSpec(memory_space=pl.ANY)
    local = pl.BlockSpec(memory_space=pltpu.VMEM)
    pair, sent, landed = pltpu.SemaphoreType.DMA((2,)), pltpu.SemaphoreType.DMA((2, CHUNKS)), pltpu.SemaphoreType.DMA((3, CHUNKS))
    part = (CHUNKS, batch, width // CHUNKS)
    new_rows = jax.ShapeDtypeStruct((rows, heads, head_dim), F32)
    return pl.pallas_call(
        functools.partial(pipeline_kernel, stages, batch),
        out_shape=(jax.ShapeDtypeStruct((rows, width), BF16), new_rows, new_rows),
        in_specs=[pl.BlockSpec(memory_space=pltpu.SMEM), local, local, local] + [anywhere] * 8,
        out_specs=(anywhere, anywhere, anywhere),
        scratch_shapes=[
            pltpu.VMEM(wqkv.shape, BF16), pltpu.VMEM(wout.shape, BF16), pltpu.VMEM(wgate.shape, BF16), pltpu.VMEM(wup.shape, BF16), pltpu.VMEM(wdown.shape, BF16),
            pltpu.VMEM((batch, slots, heads, head_dim), BF16), pltpu.VMEM((batch, slots, heads, head_dim), BF16),
            pltpu.VMEM((2, batch, width), BF16), pltpu.VMEM((2, batch, width), BF16), pltpu.VMEM((3, batch, width), F32),
            pltpu.VMEM((2,) + part, BF16), pltpu.VMEM((3,) + part, BF16), pltpu.VMEM((2,) + part, BF16), pltpu.VMEM((3,) + part, BF16),
            pltpu.VMEM((batch, width), BF16), pltpu.VMEM((batch, wgate.shape[1]), BF16), pltpu.VMEM((batch, heads * head_dim), BF16),
            pltpu.VMEM((batch, heads, head_dim), F32), pltpu.VMEM((batch, heads, head_dim), F32), pltpu.VMEM((batch, heads, head_dim), F32), pltpu.VMEM((batch, heads, head_dim), F32),
            pltpu.SemaphoreType.DMA((5,)), pair, pair, pair, sent, landed, sent, landed, pair, pair,
            pltpu.SemaphoreType.DMA((2, stages)), pltpu.SemaphoreType.DMA((count,)), pltpu.SemaphoreType.REGULAR,
        ],
        compiler_params=pltpu.CompilerParams(has_side_effects=True, vmem_limit_bytes=VMEM_LIMIT),
    )(lens, gains, cos_part, sin_part, embeds, wqkv, wout, wgate, wup, wdown, k_cache, v_cache)


def tail_kernel(lens_ref, gain_ref, final_ref, knew_ref, vnew_ref, kc_hbm, vc_hbm, wun_ref, logits_ref, ko_hbm, vo_hbm, normed, kring, vring, in_sem, out_sem):
    block = pl.program_id(0)
    steps = pl.num_programs(0)
    rows = kring.shape[1]

    def reads(step):
        slot, span = lax.rem(step, 3), pl.ds(step * rows, rows)
        return [pltpu.make_async_copy(src.at[span], ring.at[slot], in_sem.at[i, slot]) for i, (src, ring) in enumerate([(kc_hbm, kring), (vc_hbm, vring)])]

    def writes(step):
        slot, span = lax.rem(step, 3), pl.ds(step * rows, rows)
        return [pltpu.make_async_copy(ring.at[slot], dst.at[span], out_sem.at[i, slot]) for i, (dst, ring) in enumerate([(ko_hbm, kring), (vo_hbm, vring)])]

    @pl.when(block == 0)
    def _():
        for copy in reads(0) + reads(1):
            copy.start()
        normed[...] = rms_norm(final_ref[...].astype(F32), gain_ref[...])

    for copy in reads(block):
        copy.wait()
    slot = lax.rem(block, 3)

    def place(row, carry):
        length = lens_ref[block * rows + row]
        kring[slot, row, length] = knew_ref[row].astype(BF16)
        vring[slot, row, length] = vnew_ref[row].astype(BF16)
        return carry

    lax.fori_loop(0, rows, place, 0, unroll=4)
    for copy in writes(block):
        copy.start()

    @pl.when(block > 0)
    def _():
        for copy in writes(block - 1):
            copy.wait()

    @pl.when(block + 2 < steps)
    def _():
        for copy in reads(block + 2):
            copy.start()

    logits_ref[...] = lax.dot_general(normed[...], wun_ref[...], (((1,), (1,)), ((), ())), preferred_element_type=F32)

    @pl.when(block == steps - 1)
    def _():
        for copy in writes(block):
            copy.wait()


def run_tail(lens, gain, final, knew, vnew, k_cache, v_cache, wun):
    rows, width = final.shape
    slots, heads, head_dim = k_cache.shape[1:]
    vocab = wun.shape[0]
    block = rows // TAIL_STEPS
    columns = pl.cdiv(vocab, TAIL_STEPS * 128) * 128
    cache_spec = pl.BlockSpec(memory_space=pl.ANY)
    ring = pltpu.VMEM((3, block, slots, heads, head_dim), BF16)
    new_spec = pl.BlockSpec((block, heads, head_dim), lambda i, lens: (i, 0, 0))
    return pl.pallas_call(
        tail_kernel,
        out_shape=(jax.ShapeDtypeStruct((rows, vocab), F32), jax.ShapeDtypeStruct(k_cache.shape, BF16), jax.ShapeDtypeStruct(v_cache.shape, BF16)),
        grid_spec=pltpu.PrefetchScalarGridSpec(
            num_scalar_prefetch=1,
            grid=(TAIL_STEPS,),
            in_specs=[pl.BlockSpec((1, width), lambda i, lens: (0, 0)), pl.BlockSpec((rows, width), lambda i, lens: (0, 0)), new_spec, new_spec, cache_spec, cache_spec,
                      pl.BlockSpec((columns, width), lambda i, lens: (i, 0))],
            out_specs=(pl.BlockSpec((rows, columns), lambda i, lens: (0, i)), cache_spec, cache_spec),
            scratch_shapes=[pltpu.VMEM((rows, width), BF16), ring, ring, pltpu.SemaphoreType.DMA((2, 3)), pltpu.SemaphoreType.DMA((2, 3))],
        ),
        compiler_params=pltpu.CompilerParams(dimension_semantics=("arbitrary",), vmem_limit_bytes=VMEM_LIMIT),
    )(lens, gain, final, knew, vnew, k_cache, v_cache, wun)


def solution(mesh):
    stages = mesh.shape['stage']
    cache_spec = P('stage', 'replica', None, None, 'tp', None)
    in_specs = (P('replica'), P('stage', None, 'tp', None, None), P('stage', 'tp', None), P('stage', None, 'tp'), P('stage', None, 'tp'), P('stage', 'tp', None), P('stage'), cache_spec, cache_spec, P('replica'), P(), P(None, ('stage', 'tp')))
    out_specs = (P('replica', None, ('stage', 'tp')), cache_spec, cache_spec)

    def device_step(embeds, w_qkv, w_out, w_gate, w_up, w_down, norm_gain, k_cache, v_cache, lengths, final_gain, w_unembed):
        groups, seqs, width = embeds.shape
        rows = groups * seqs
        cache_shape = k_cache.shape
        head_dim = cache_shape[-1]
        lens = lengths.reshape(rows)
        cos_part, sin_part = rope_tables(lens, head_dim)
        k_rows = k_cache.reshape((rows,) + cache_shape[3:])
        v_rows = v_cache.reshape((rows,) + cache_shape[3:])
        final, knew, vnew = run_pipeline(
            stages, lens, norm_gain[0], cos_part, sin_part, embeds.reshape(rows, width), w_qkv[0].transpose(0, 2, 1, 3).reshape(width, -1), w_out[0], w_gate[0], w_up[0], w_down[0], k_rows, v_rows)
        logits, k_out, v_out = run_tail(lens, final_gain.reshape(1, width), final, knew, vnew, k_rows, v_rows, w_unembed.T)
        return logits.reshape(groups, seqs, -1), k_out.reshape(cache_shape), v_out.reshape(cache_shape)

    return jax.shard_map(device_step, mesh=mesh, in_specs=in_specs, out_specs=out_specs, check_vma=False)
```

```python
import functools

import jax
import jax.numpy as jnp
from jax import lax
from jax.experimental import pallas as pl
from jax.experimental.pallas import tpu as pltpu
from jax.sharding import PartitionSpec as P

NORM_EPS = 1e-5
ROPE_THETA = 10000.0
MESH = pl.DeviceIdType.MESH
F32 = jnp.float32
BF16 = jnp.bfloat16
MERGE = 4
TAIL_STEPS = 16
LOG2_E = 1.4426950408889634
ROW_UNROLL = 16
CHUNKS = 2
TILE = 256
VMEM_LIMIT = 67043328


def rms_norm(values, gain_row):
    mean_sq = jnp.mean(values * values, axis=-1, keepdims=True)
    return (values * lax.rsqrt(mean_sq + NORM_EPS) * gain_row).astype(BF16)


def rope_tables(lengths, head_dim):
    inv_freq = ROPE_THETA ** (-jnp.arange(head_dim // 2, dtype=F32) * (2.0 / head_dim))
    angles = lengths.astype(F32)[..., None] * inv_freq
    cos_part, sin_part = jnp.cos(angles), jnp.sin(angles)
    return jnp.concatenate([cos_part, cos_part], -1), jnp.concatenate([-sin_part, sin_part], -1)


def column_chunks(total, width):
    return [(low, min(width, total - low)) for low in range(0, total, width)]


def joined(ref, slot):
    return jnp.concatenate([ref[slot, chunk].astype(F32) for chunk in range(CHUNKS)], axis=-1)


def dot(lhs, rhs):
    return jnp.dot(lhs, rhs, preferred_element_type=F32)


def pipeline_kernel(
    stages, batch, lens_ref, gain_ref, cos_ref, sin_ref, emb_ref, wqkv_hbm, wout_hbm, wgate_hbm, wup_hbm, wdown_hbm, kc_hbm, vc_hbm,
    final_ref, knew_ref, vnew_ref,
    wqkv, wout, wgate, wup, wdown, kbuf, vbuf, xbuf, xout, resid, send_a, recv_a, send_d, recv_d, unit, hidden, attn, q_scr, k_scr, v_scr, o_scr, eye,
    w_sem, t_sem, c_sem, n_sem, e_sem, a_send, a_recv, d_send, d_recv, x_send, x_recv, f_send, f_recv, credit,
):
    stage = lax.axis_index("stage")
    peer = {"tp": 1 - lax.axis_index("tp")}
    last = stages - 1
    rows = emb_ref.shape[0]
    count = rows // batch
    heads, head_dim = kbuf.shape[2], kbuf.shape[3]
    slots = kbuf.shape[1]
    scale = head_dim ** -0.5
    weights = [pltpu.make_async_copy(src, dst, w_sem.at[i]) for i, (src, dst) in enumerate([(wqkv_hbm, wqkv), (wout_hbm, wout)])]
    whole, rest = divmod(wdown.shape[0], TILE)

    def block_copy(src, index, size=TILE):
        lines = pl.ds(index * TILE, size)
        return pltpu.make_async_copy(src.at[lines], wdown.at[lines], t_sem.at[index])

    def each_block(action):
        def body(index, carry):
            action(pl.multiple_of(index * TILE, TILE), index, TILE)
            return carry

        lax.fori_loop(0, whole, body, 0)
        if rest:
            action(whole * TILE, whole, rest)

    def turn(src, dst, following):
        def action(low, index, size):
            block_copy(src, index, size).wait()
            for col in range(0, wdown.shape[1], TILE):
                turned = lax.dot_general(eye[...], wdown[pl.ds(low, size), col:col + TILE], (((1,), (1,)), ((), ())), preferred_element_type=F32)
                dst[col:col + TILE, pl.ds(low, size)] = turned.astype(BF16)
            block_copy(following, index, size).start()

        each_block(action)

    def span(step):
        return pl.ds(pl.multiple_of(step * batch, batch), batch)

    def emb_copy(step):
        return pltpu.make_async_copy(emb_ref.at[span(step)], xbuf.at[lax.rem(step, 2)], e_sem.at[lax.rem(step, 2)])

    def cache_copies(step):
        return (pltpu.make_async_copy(kc_hbm.at[span(step)], kbuf, c_sem.at[0]), pltpu.make_async_copy(vc_hbm.at[span(step)], vbuf, c_sem.at[1]))

    def new_copies(step):
        return (pltpu.make_async_copy(k_scr, knew_ref.at[span(step)], n_sem.at[0]), pltpu.make_async_copy(v_scr, vnew_ref.at[span(step)], n_sem.at[1]))

    def sum_copy(step, chunk, send, recv, send_sem, recv_sem):
        out, into = lax.rem(step, 2), lax.rem(step, 3)
        return pltpu.make_async_remote_copy(send.at[out, chunk], recv.at[into, chunk], send_sem.at[out, chunk], recv_sem.at[into, chunk], device_id=peer, device_id_type=MESH)

    def hop_copy(step):
        slot = lax.rem(step, 2)
        return pltpu.make_async_remote_copy(xout.at[slot], xbuf.at[slot], x_send.at[slot], x_recv.at[slot], device_id={"stage": stage + 1}, device_id_type=MESH)

    def final_copies(step):
        slot = lax.rem(step, 2)
        return [pltpu.make_async_remote_copy(xout.at[slot], final_ref.at[span(step)], f_send.at[slot, dst], f_recv.at[step], device_id={"stage": dst}, device_id_type=MESH)
                for dst in range(last)]

    def final_local(step):
        slot = lax.rem(step, 2)
        return pltpu.make_async_copy(xout.at[slot], final_ref.at[span(step)], f_send.at[slot, last])

    each_block(lambda low, index, size: block_copy(wgate_hbm, index, size).start())
    for copy in weights[:1] + list(cache_copies(0)) + weights[1:]:
        copy.start()

    @pl.when(stage == 0)
    def _():
        emb_copy(0).start()
        emb_copy(1).start()

    def attend(step):
        slot = lax.rem(step, 2)

        @pl.when(stage == 0)
        def _():
            emb_copy(step).wait()

        @pl.when(stage > 0)
        def _():
            pltpu.make_async_remote_copy(xout.at[slot], xbuf.at[slot], x_send.at[slot], x_recv.at[slot], device_id={"stage": stage}, device_id_type=MESH).wait_recv()

        @pl.when(step == 0)
        def _():
            weights[0].wait()

        @pl.when(step > 0)
        def _():
            for copy in new_copies(step - 1):
                copy.wait()

        unit[...] = rms_norm(xbuf[slot].astype(F32), gain_ref[0:1, :])
        cos_part = cos_ref[span(step), :]
        sin_part = sin_ref[span(step), :]
        for low, width in column_chunks(wqkv.shape[1], 8 * head_dim):
            proj = dot(unit[...], wqkv[:, low:low + width])
            for part in range(width // head_dim):
                kind, head = divmod(low // head_dim + part, heads)
                piece = proj[:, part * head_dim:(part + 1) * head_dim]
                if kind < 2:
                    piece = piece * cos_part + pltpu.roll(piece, head_dim // 2, 1) * sin_part
                (q_scr, k_scr, v_scr)[kind][:, head, :] = piece.astype(BF16).astype(F32)
        for copy in cache_copies(step):
            copy.wait()
        for copy in new_copies(step):
            copy.start()
        used = slots - 1
        lane = lax.broadcasted_iota(jnp.int32, (heads, head_dim), 1)

        def score_rows(index, carry):
            group = pl.ds(index * ROW_UNROLL, ROW_UNROLL)
            query = q_scr[group] * (scale * LOG2_E)
            packed = jnp.where(lane == used, jnp.sum(query * k_scr[group], axis=-1, keepdims=True), -jnp.inf)
            for slot_idx in range(used):
                packed = jnp.where(lane == slot_idx, jnp.sum(query * kbuf[group, slot_idx].astype(F32), axis=-1, keepdims=True), packed)
            for sub in range(ROW_UNROLL):
                length = lens_ref[step * batch + index * ROW_UNROLL + sub]
                q_scr[index * ROW_UNROLL + sub] = jnp.where(jnp.logical_or(lane < length, lane == used), packed[sub], -jnp.inf)
            return carry

        lax.fori_loop(0, batch // ROW_UNROLL, score_rows, 0)
        packed = q_scr[...]
        exps = jnp.exp2(packed - jnp.max(packed, axis=-1, keepdims=True))
        q_scr[...] = (exps * (1.0 / jnp.sum(exps, axis=-1, keepdims=True))).astype(BF16).astype(F32)

        def value_rows(index, carry):
            group = pl.ds(index * ROW_UNROLL, ROW_UNROLL)
            probs = q_scr[group]
            total = probs[:, :, used:used + 1] * v_scr[group]
            for slot_idx in range(used):
                total = total + probs[:, :, slot_idx:slot_idx + 1] * vbuf[group, slot_idx].astype(F32)
            o_scr[group] = total
            return carry

        lax.fori_loop(0, batch // ROW_UNROLL, value_rows, 0)

        @pl.when(step + 1 < count)
        def _():
            for copy in cache_copies(step + 1):
                copy.start()

    def project(step):
        slot = lax.rem(step, 2)

        @pl.when(step == 0)
        def _():
            weights[1].wait()

        for head in range(heads):
            attn[:, head * head_dim:(head + 1) * head_dim] = o_scr[:, head, :].astype(BF16)
        for chunk, (low, width) in enumerate(column_chunks(wout.shape[1], wout.shape[1] // CHUNKS)):
            partial = dot(attn[...], wout[:, low:low + width])
            send_a[slot, chunk] = partial.astype(BF16)
            resid[lax.rem(step, 3), :, low:low + width] = xbuf[slot, :, low:low + width].astype(F32) + partial
            sum_copy(step, chunk, send_a, recv_a, a_send, a_recv).start()

        @pl.when(jnp.logical_and(stage == 0, step + 2 < count))
        def _():
            emb_copy(step + 2).start()

        @pl.when(jnp.logical_and(stage > 0, step + 2 < count))
        def _():
            pl.semaphore_signal(credit, inc=1, device_id={"stage": stage - 1}, device_id_type=MESH)

    def feed_forward(step):
        slot = lax.rem(step, 2)

        @pl.when(step == 0)
        def _():
            each_block(lambda low, index, size: block_copy(wdown_hbm, index, size).wait())

        kept = lax.rem(step, 3)
        for chunk in range(CHUNKS):
            sum_copy(step, chunk, send_a, recv_a, a_send, a_recv).wait()
        summed = resid[kept] + joined(recv_a, kept)
        resid[kept] = summed
        unit[...] = rms_norm(summed, gain_ref[1:2, :])
        for low, width in column_chunks(wgate.shape[1], 768):
            gate = dot(unit[...], wgate[:, low:low + width])
            up = dot(unit[...], wup[:, low:low + width])
            hidden[:, low:low + width] = (jax.nn.silu(gate) * up).astype(BF16)
        for chunk, (low, width) in enumerate(column_chunks(wdown.shape[1], wdown.shape[1] // CHUNKS)):
            partial = dot(hidden[...], wdown[:, low:low + width])
            send_d[slot, chunk] = partial.astype(BF16)
            resid[kept, :, low:low + width] = resid[kept, :, low:low + width] + partial
            sum_copy(step, chunk, send_d, recv_d, d_send, d_recv).start()

    def hand_on(step):
        slot = lax.rem(step, 2)
        for chunk in range(CHUNKS):
            sum_copy(step, chunk, send_d, recv_d, d_send, d_recv).wait()

        @pl.when(jnp.logical_and(stage < last, step >= 2))
        def _():
            hop_copy(step - 2).wait_send()
            pl.semaphore_wait(credit, 1)

        @pl.when(jnp.logical_and(stage == last, step >= 2))
        def _():
            for copy in final_copies(step - 2):
                copy.wait_send()
            final_local(step - 2).wait()

        kept = lax.rem(step, 3)
        xout[slot] = (resid[kept] + joined(recv_d, kept)).astype(BF16)

        @pl.when(stage < last)
        def _():
            hop_copy(step).start()

        @pl.when(stage == last)
        def _():
            for copy in final_copies(step):
                copy.start()
            final_local(step).start()

    def slot_body(step, carry):
        @pl.when(step < count)
        def _():
            attend(step)

        @pl.when(step < count)
        def _():
            project(step)

        @pl.when(step >= 2)
        def _():
            hand_on(step - 2)

        @pl.when(jnp.logical_and(step >= 1, step <= count))
        def _():
            feed_forward(step - 1)

        return carry

    eye[...] = (lax.broadcasted_iota(jnp.int32, eye.shape, 0) == lax.broadcasted_iota(jnp.int32, eye.shape, 1)).astype(F32).astype(BF16)
    turn(wgate_hbm, wgate, wup_hbm)
    turn(wup_hbm, wup, wdown_hbm)
    lax.fori_loop(0, count + 2, slot_body, 0)
    for copy in new_copies(count - 1):
        copy.wait()

    @pl.when(stage < last)
    def _():
        for step in (count - 2, count - 1):
            hop_copy(step).wait_send()

        def drain(step, carry):
            pltpu.make_async_remote_copy(xout.at[0], final_ref.at[span(step)], f_send.at[0, 0], f_recv.at[step], device_id={"stage": stage}, device_id_type=MESH).wait_recv()
            return carry

        lax.fori_loop(0, count, drain, 0)

    @pl.when(stage == last)
    def _():
        for step in (count - 2, count - 1):
            for copy in final_copies(step):
                copy.wait_send()
            final_local(step).wait()


def run_pipeline(stages, lens, gains, cos_part, sin_part, embeds, wqkv, wout, wgate, wup, wdown, k_cache, v_cache):
    rows, width = embeds.shape
    batch = 16 * MERGE
    slots, heads, head_dim = k_cache.shape[1:]
    count = rows // batch
    anywhere = pl.BlockSpec(memory_space=pl.ANY)
    local = pl.BlockSpec(memory_space=pltpu.VMEM)
    pair, sent, landed = pltpu.SemaphoreType.DMA((2,)), pltpu.SemaphoreType.DMA((2, CHUNKS)), pltpu.SemaphoreType.DMA((3, CHUNKS))
    part = (CHUNKS, batch, width // CHUNKS)
    new_rows = jax.ShapeDtypeStruct((rows, heads, head_dim), F32)
    return pl.pallas_call(
        functools.partial(pipeline_kernel, stages, batch),
        out_shape=(jax.ShapeDtypeStruct((rows, width), BF16), new_rows, new_rows),
        in_specs=[pl.BlockSpec(memory_space=pltpu.SMEM), local, local, local] + [anywhere] * 8,
        out_specs=(anywhere, anywhere, anywhere),
        scratch_shapes=[
            pltpu.VMEM(wqkv.shape, BF16), pltpu.VMEM(wout.shape, BF16), pltpu.VMEM(wgate.shape[::-1], BF16), pltpu.VMEM(wup.shape[::-1], BF16), pltpu.VMEM(wdown.shape, BF16),
            pltpu.VMEM((batch, slots, heads, head_dim), BF16), pltpu.VMEM((batch, slots, heads, head_dim), BF16),
            pltpu.VMEM((2, batch, width), BF16), pltpu.VMEM((2, batch, width), BF16), pltpu.VMEM((3, batch, width), F32),
            pltpu.VMEM((2,) + part, BF16), pltpu.VMEM((3,) + part, BF16), pltpu.VMEM((2,) + part, BF16), pltpu.VMEM((3,) + part, BF16),
            pltpu.VMEM((batch, width), BF16), pltpu.VMEM((batch, wdown.shape[0]), BF16), pltpu.VMEM((batch, heads * head_dim), BF16),
            pltpu.VMEM((batch, heads, head_dim), F32), pltpu.VMEM((batch, heads, head_dim), F32), pltpu.VMEM((batch, heads, head_dim), F32), pltpu.VMEM((batch, heads, head_dim), F32), pltpu.VMEM((TILE, TILE), BF16),
            pair, pltpu.SemaphoreType.DMA((pl.cdiv(wdown.shape[0], TILE),)), pair, pair, pair, sent, landed, sent, landed, pair, pair,
            pltpu.SemaphoreType.DMA((2, stages)), pltpu.SemaphoreType.DMA((count,)), pltpu.SemaphoreType.REGULAR,
        ],
        compiler_params=pltpu.CompilerParams(has_side_effects=True, vmem_limit_bytes=VMEM_LIMIT),
    )(lens, gains, cos_part, sin_part, embeds, wqkv, wout, wgate, wup, wdown, k_cache, v_cache)


def tail_kernel(lens_ref, gain_ref, final_ref, knew_ref, vnew_ref, kc_hbm, vc_hbm, wun_ref, logits_ref, ko_hbm, vo_hbm, normed, kring, vring, in_sem, out_sem):
    block = pl.program_id(0)
    steps = pl.num_programs(0)
    rows = kring.shape[1]

    def reads(step):
        slot, span = lax.rem(step, 3), pl.ds(step * rows, rows)
        return [pltpu.make_async_copy(src.at[span], ring.at[slot], in_sem.at[i, slot]) for i, (src, ring) in enumerate([(kc_hbm, kring), (vc_hbm, vring)])]

    def writes(step):
        slot, span = lax.rem(step, 3), pl.ds(step * rows, rows)
        return [pltpu.make_async_copy(ring.at[slot], dst.at[span], out_sem.at[i, slot]) for i, (dst, ring) in enumerate([(ko_hbm, kring), (vo_hbm, vring)])]

    @pl.when(block == 0)
    def _():
        for copy in reads(0) + reads(1):
            copy.start()
        normed[...] = rms_norm(final_ref[...].astype(F32), gain_ref[...])

    for copy in reads(block):
        copy.wait()
    slot = lax.rem(block, 3)

    def place(row, carry):
        length = lens_ref[block * rows + row]
        kring[slot, row, length] = knew_ref[row].astype(BF16)
        vring[slot, row, length] = vnew_ref[row].astype(BF16)
        return carry

    lax.fori_loop(0, rows, place, 0, unroll=4)
    for copy in writes(block):
        copy.start()

    @pl.when(block > 0)
    def _():
        for copy in writes(block - 1):
            copy.wait()

    @pl.when(block + 2 < steps)
    def _():
        for copy in reads(block + 2):
            copy.start()

    logits_ref[...] = lax.dot_general(normed[...], wun_ref[...], (((1,), (1,)), ((), ())), preferred_element_type=F32)

    @pl.when(block == steps - 1)
    def _():
        for copy in writes(block):
            copy.wait()


def run_tail(lens, gain, final, knew, vnew, k_cache, v_cache, wun):
    rows, width = final.shape
    slots, heads, head_dim = k_cache.shape[1:]
    vocab = wun.shape[0]
    block = rows // TAIL_STEPS
    columns = pl.cdiv(vocab, TAIL_STEPS * 128) * 128
    cache_spec = pl.BlockSpec(memory_space=pl.ANY)
    ring = pltpu.VMEM((3, block, slots, heads, head_dim), BF16)
    new_spec = pl.BlockSpec((block, heads, head_dim), lambda i, lens: (i, 0, 0))
    return pl.pallas_call(
        tail_kernel,
        out_shape=(jax.ShapeDtypeStruct((rows, vocab), F32), jax.ShapeDtypeStruct(k_cache.shape, BF16), jax.ShapeDtypeStruct(v_cache.shape, BF16)),
        grid_spec=pltpu.PrefetchScalarGridSpec(
            num_scalar_prefetch=1,
            grid=(TAIL_STEPS,),
            in_specs=[pl.BlockSpec((1, width), lambda i, lens: (0, 0)), pl.BlockSpec((rows, width), lambda i, lens: (0, 0)), new_spec, new_spec, cache_spec, cache_spec,
                      pl.BlockSpec((columns, width), lambda i, lens: (i, 0))],
            out_specs=(pl.BlockSpec((rows, columns), lambda i, lens: (0, i)), cache_spec, cache_spec),
            scratch_shapes=[pltpu.VMEM((rows, width), BF16), ring, ring, pltpu.SemaphoreType.DMA((2, 3)), pltpu.SemaphoreType.DMA((2, 3))],
        ),
        compiler_params=pltpu.CompilerParams(dimension_semantics=("arbitrary",), vmem_limit_bytes=VMEM_LIMIT),
    )(lens, gain, final, knew, vnew, k_cache, v_cache, wun)


def solution(mesh):
    stages = mesh.shape['stage']
    cache_spec = P('stage', 'replica', None, None, 'tp', None)
    in_specs = (P('replica'), P('stage', None, 'tp', None, None), P('stage', 'tp', None), P('stage', None, 'tp'), P('stage', None, 'tp'), P('stage', 'tp', None), P('stage'), cache_spec, cache_spec, P('replica'), P(), P(None, ('stage', 'tp')))
    out_specs = (P('replica', None, ('stage', 'tp')), cache_spec, cache_spec)

    def device_step(embeds, w_qkv, w_out, w_gate, w_up, w_down, norm_gain, k_cache, v_cache, lengths, final_gain, w_unembed):
        groups, seqs, width = embeds.shape
        rows = groups * seqs
        cache_shape = k_cache.shape
        head_dim = cache_shape[-1]
        lens = lengths.reshape(rows)
        cos_part, sin_part = rope_tables(lens, head_dim)
        k_rows = k_cache.reshape((rows,) + cache_shape[3:])
        v_rows = v_cache.reshape((rows,) + cache_shape[3:])
        final, knew, vnew = run_pipeline(
            stages, lens, norm_gain[0], cos_part, sin_part, embeds.reshape(rows, width), w_qkv[0].transpose(0, 2, 1, 3).reshape(width, -1), w_out[0], w_gate[0].T, w_up[0].T, w_down[0], k_rows, v_rows)
        logits, k_out, v_out = run_tail(lens, final_gain.reshape(1, width), final, knew, vnew, k_rows, v_rows, w_unembed.T)
        return logits.reshape(groups, seqs, -1), k_out.reshape(cache_shape), v_out.reshape(cache_shape)

    return jax.shard_map(device_step, mesh=mesh, in_specs=in_specs, out_specs=out_specs, check_vma=False)
```
